512 devices in a mesh: row: 32 (over z, x_lo, core), col: 16 (over y, x_hi).
Axes of the slice: x: 4 (x_hi: 2, x_lo: 2; x = x_hi * 2 + x_lo), y: 8, z: 8, core: 2. Of those that a mesh axis runs over, the one named last changes fastest.
Arguments:
- substrate: float32 [4096, 4096], P('row', 'col'), may hold values from 0.05 to 0.95
- activator: float32 [4096, 4096], P('row', 'col'), may hold values from 0 to 0.45
Outputs:
- substrate_section: float32 [4096, 4096], P('row', 'col')
- activator_section: float32 [4096, 4096], P('row', 'col')
The draws below stay inside these ranges and needn't reach their ends.
All inputs are finite; a program needn't handle non-finite values.
Results may differ from the reference program's by a relative error of at most 0.00023.
Values sent between devices are 32-bit elements; how exact they have to be, the bound alone decides.
A program may use at most 64 MiB of HBM per device.

```python
import math
import jax
import jax.numpy as jnp

NX = 4096
NY = 4096


def smooth_part(key):
    orders = jnp.arange(1, 5, dtype=jnp.float32)
    row_coords = jnp.arange(NX, dtype=jnp.float32) / NX
    col_coords = jnp.arange(NY, dtype=jnp.float32) / NY
    row_angles = 2.0 * math.pi * orders[:, None] * row_coords[None, :]
    col_angles = 2.0 * math.pi * orders[:, None] * col_coords[None, :]
    basis_rows = jnp.concatenate([jnp.cos(row_angles), jnp.sin(row_angles)], axis=0)
    basis_cols = jnp.concatenate([jnp.cos(col_angles), jnp.sin(col_angles)], axis=0)
    coefficients = jax.random.normal(key, (8, 8), jnp.float32)
    mixed = jnp.dot(coefficients, basis_cols, preferred_element_type=jnp.float32)
    return jnp.dot(basis_rows.T, mixed, preferred_element_type=jnp.float32) / 4.0


def draw_substrate(key, part):
    smooth = smooth_part(jax.random.fold_in(key, 11))
    rough_key = jax.random.fold_in(key, 12)
    rough_part = jax.random.uniform(rough_key, (NX, NY), jnp.float32, -1.0, 1.0)
    return (0.55 + 0.2 * jnp.tanh(smooth) + 0.15 * rough_part).astype(jnp.float32)


def draw_activator(key, part):
    smooth = smooth_part(jax.random.fold_in(key, 23))
    rough_key = jax.random.fold_in(key, 24)
    rough_part = jax.random.uniform(rough_key, (NX, NY), jnp.float32, -1.0, 1.0)
    return (0.25 + 0.08 * jnp.tanh(smooth) + 0.08 * rough_part).astype(jnp.float32)


def setup_inputs(seed: int = 0) -> dict:
    key_of = jax.random.split(jax.random.key(seed), 3)
    substrate = draw_substrate(jax.random.fold_in(key_of[2], 71), 0)
    activator = draw_activator(jax.random.fold_in(key_of[2], 71), 0)
    return dict(substrate=substrate, activator=activator)


FEED_RATE = 0.037
KILL_RATE = 0.06
TIME_STEP = 8.0
SUBSTRATE_DIFFUSION = 4e-7
ACTIVATOR_DIFFUSION = 2e-7


def signed_squares(total):
    indices = jnp.arange(total, dtype=jnp.int32)
    signed = jnp.where(2 * indices < total, indices, indices - total).astype(jnp.float32)
    angular = (2.0 * math.pi) * signed
    return angular * angular


def section_factors(wave_number, diffusion, decay_rate):
    linear = -diffusion * wave_number - decay_rate
    exponent = linear * (0.5 * TIME_STEP)
    return jnp.exp(exponent), jnp.expm1(exponent) / linear


def species_section(field, source, wave_number, diffusion, decay_rate):
    growth, forcing = section_factors(wave_number, diffusion, decay_rate)
    spectrum = jnp.fft.fft2(field + 1j * source)
    advanced = spectrum * (growth - 1j * forcing)
    return jnp.real(jnp.fft.ifft2(advanced)).astype(jnp.float32)


def reference(substrate, activator):
    reaction = substrate * activator * activator
    wave_number = signed_squares(NX)[:, None] + signed_squares(NY)[None, :]
    substrate_section = species_section(substrate, FEED_RATE - reaction, wave_number, SUBSTRATE_DIFFUSION, FEED_RATE)
    activator_section = species_section(activator, reaction, wave_number, ACTIVATOR_DIFFUSION, FEED_RATE + KILL_RATE)
    return (substrate_section, activator_section)
```

```python
import math

import jax
import jax.numpy as jnp
import numpy as np
from jax import lax
from jax.experimental import pallas as pl
from jax.experimental.pallas import tpu as pltpu
from jax.sharding import PartitionSpec as P

FEED_RATE = 0.037
KILL_RATE = 0.06
HALF_STEP = 4.0
SUBSTRATE = (4e-07, FEED_RATE)
ACTIVATOR = (2e-07, FEED_RATE + KILL_RATE)
TOTAL = 4096
COLS = 16
ROWS = 32
WIDE = 256
LANES = 128
F32 = jnp.float32
BF16 = jnp.bfloat16


def c_add(a, b):
    im = a[1] if b[1] is None else (b[1] if a[1] is None else a[1] + b[1])
    return (a[0] + b[0], im)


def c_sub(a, b):
    im = a[1] if b[1] is None else (-b[1] if a[1] is None else a[1] - b[1])
    return (a[0] - b[0], im)


def c_conj(a):
    return (a[0], None if a[1] is None else -a[1])


def c_turn(a, numerator, denominator):
    numerator %= denominator
    if numerator == 0:
        return a
    if 4 * numerator == denominator:
        return (jnp.zeros_like(a[0]) if a[1] is None else -a[1], a[0])
    if 4 * numerator == 3 * denominator:
        return (jnp.zeros_like(a[0]) if a[1] is None else a[1], -a[0])
    cosine = math.cos(2.0 * math.pi * numerator / denominator)
    sine = math.sin(2.0 * math.pi * numerator / denominator)
    if a[1] is None:
        return (a[0] * cosine, a[0] * sine)
    return (a[0] * cosine - a[1] * sine, a[0] * sine + a[1] * cosine)


def real_forward(values):
    size = len(values)
    if size == 2:
        return [(values[0] + values[1], None), (values[0] - values[1], None)]
    even, odd = real_forward(values[::2]), real_forward(values[1::2])
    return join_halves(even, odd, size)


def join_halves(even, odd, size, first=0):
    half = size // 2
    out = [None] * (half + 1)
    for k in range(first, half // 2 + 1):
        turned = c_turn(odd[k], -k, size)
        out[k] = c_add(even[k], turned)
        if half - k != k:
            out[half - k] = c_conj(c_sub(even[k], turned))
    return out


def split_halves(spectrum, size, first=0):
    half = size // 2
    even, odd = [None] * (half // 2 + 1), [None] * (half // 2 + 1)
    for k in range(first, half // 2 + 1):
        if k == 0:
            even[k] = (spectrum[0][0] + spectrum[half][0], None)
            odd[k] = (spectrum[0][0] - spectrum[half][0], None)
        elif 2 * k == half:
            even[k] = (2.0 * spectrum[k][0], None)
            odd[k] = (-2.0 * spectrum[k][1], None)
        else:
            other = c_conj(spectrum[half - k])
            even[k] = c_add(spectrum[k], other)
            odd[k] = c_turn(c_sub(spectrum[k], other), k, size)
    return even, odd


def real_backward(spectrum):
    size = 2 * (len(spectrum) - 1)
    if size == 2:
        a, b = spectrum[0][0], spectrum[1][0]
        return [a + b, a - b]
    even, odd = split_halves(spectrum, size)
    even, odd = real_backward(even), real_backward(odd)
    return [x for pair in zip(even, odd) for x in pair]


def roll_rows(tile, shift):
    return pltpu.roll(tile, shift, 0)


def sublane():
    return lax.broadcasted_iota(jnp.int32, (8, LANES), 0)


def part_sign():
    return jnp.where(sublane() < 4, 1.0, -1.0).astype(F32)


def tile_turn(tile, sign, cosine, sine):
    return tile * cosine - (sign * sine) * roll_rows(tile, 4)


def tile_fft(tiles, sign, direction):
    size = len(tiles)
    if size == 1:
        return tiles
    even, odd = tile_fft(tiles[::2], sign, direction), tile_fft(tiles[1::2], sign, direction)
    low, high = [], []
    for k in range(size // 2):
        turned = odd[k]
        if 4 * k == size:
            turned = (-direction * sign) * roll_rows(turned, 4)
        elif k:
            angle = direction * 2.0 * math.pi * k / size
            turned = tile_turn(turned, sign, math.cos(angle), math.sin(angle))
        low.append(even[k] + turned)
        high.append(even[k] - turned)
    return low + high


def dot3(values, high, low, dims):
    dot = lambda a, b: lax.dot_general(a, b, (dims, ((), ())), preferred_element_type=F32)
    top = values.astype(BF16)
    rest = (values - top.astype(F32)).astype(BF16)
    return dot(top, high) + (dot(rest, high) + dot(top, low))


FORWARD = ((1,), (0,))
BACKWARD = ((1,), (1,))


def forward_columns(values, turn_cos, turn_sin, weights):
    even, odd = real_forward(values[::2]), real_forward(values[1::2])
    spectrum = join_halves(even, odd, COLS, 1)
    rows = [jnp.concatenate([even[0][0], odd[0][0]], axis=1)]
    for k in range(1, COLS // 2):
        re, im = spectrum[k]
        cosine, sine = turn_cos[k : k + 1, :], turn_sin[k : k + 1, :]
        rows.append(jnp.concatenate([re * cosine + im * sine, im * cosine - re * sine], axis=1))
    stacked = jnp.concatenate(rows, axis=0)
    out = dot3(stacked, weights[0], weights[1], FORWARD)
    first = dot3(stacked[:16], weights[2], weights[3], FORWARD)
    blocks = []
    for slot in range(COLS // 2):
        row = first[:8] if slot == 0 else out[8 * slot : 8 * slot + 8]
        blocks += [row[:, :WIDE], row[:, WIDE:]]
    return blocks


def backward_columns(blocks, turn_cos, turn_sin, weights):
    stacked = jnp.concatenate(
        [jnp.concatenate([blocks[2 * s], blocks[2 * s + 1]], axis=1) for s in range(COLS // 2)],
        axis=0,
    )
    out = dot3(stacked, weights[0], weights[1], BACKWARD)
    first = dot3(stacked[:16], weights[2], weights[3], BACKWARD)
    spectrum = [None] * (COLS // 2)
    for k in range(1, COLS // 2):
        row = out[8 * k : 8 * k + 8]
        re, im = row[:, :WIDE], row[:, WIDE:]
        cosine, sine = turn_cos[k : k + 1, :], turn_sin[k : k + 1, :]
        spectrum[k] = (re * cosine - im * sine, im * cosine + re * sine)
    even, odd = split_halves(spectrum + [None], COLS, 1)
    even[0], odd[0] = (first[:8, :WIDE], None), (first[:8, WIDE:], None)
    even, odd = real_backward(even), real_backward(odd)
    return [x for pair in zip(even, odd) for x in pair]


def squared_wave(index):
    signed = jnp.where(2 * index < TOTAL, index, index - TOTAL).astype(F32)
    angular = (2.0 * math.pi) * signed
    return angular * angular


def growth_forcing(wave_number, diffusion, decay_rate):
    linear = -diffusion * wave_number - decay_rate
    growth = jnp.exp(HALF_STEP * linear)
    return growth, (growth - 1.0) / linear


def factors(step, row, col):
    column = sublane() % 4
    slot, half = col // 2, col % 2
    within = LANES * half + 4 * row + column
    q = jnp.where(slot == 0, 8 * within, slot + COLS * within)
    p = step + ROWS * lax.broadcasted_iota(jnp.int32, (8, LANES), 1)
    row_wave = squared_wave(p)
    wave_number = row_wave + squared_wave(q)
    norm = 1.0 / (TOTAL * TOTAL)
    paired = jnp.where(q == 0, 1.0, jnp.where(slot == 0, 2.0, 1.0)).astype(F32)
    scale = paired * norm
    growth_s, forcing_s = growth_forcing(wave_number, *SUBSTRATE)
    growth_a, forcing_a = growth_forcing(wave_number, *ACTIVATOR)
    last = row_wave + (2.0 * math.pi * (TOTAL // 2)) ** 2
    first = column == 0
    growth_e, forcing_e = growth_forcing(
        last,
        jnp.where(first, SUBSTRATE[0], ACTIVATOR[0]).astype(F32),
        jnp.where(first, SUBSTRATE[1], ACTIVATOR[1]).astype(F32),
    )
    signed = jnp.where(first, -norm, norm).astype(F32)
    return (
        growth_s * scale,
        forcing_s * scale,
        growth_a * scale,
        forcing_a * scale,
        growth_e * norm,
        forcing_e * signed,
    )


def advance(substrate, activator, reaction, tables):
    growth_s, forcing_s, growth_a, forcing_a, growth_e, forcing_e = tables
    first = sublane() % 4 == 0
    both = jnp.where(first, substrate, roll_rows(activator, 1))
    source = jnp.where(first, reaction, roll_rows(reaction, 1))
    return (
        growth_s * substrate - forcing_s * reaction,
        growth_a * activator + forcing_a * reaction,
        growth_e * both + forcing_e * source,
    )


def constants():
    def split(matrix):
        high = matrix.astype(np.float32).astype(BF16)
        return high, (matrix - high.astype(np.float64)).astype(np.float32).astype(BF16)

    def interleave(re, im):
        size = re.shape[0]
        return np.stack([re.reshape(size, -1, 4), im.reshape(size, -1, 4)], axis=2).reshape(size, -1)

    j = np.arange(WIDE)
    angle = 2.0 * np.pi * (np.outer(j, j) % WIDE) / WIDE
    cos, sin = np.cos(angle), np.sin(angle)
    pair = interleave(np.concatenate([cos, sin]), np.concatenate([-sin, cos]))
    long = np.arange(2 * WIDE)
    angle = 2.0 * np.pi * (np.outer(long, j) % (2 * WIDE)) / (2 * WIDE)
    cos, sin = np.cos(angle), -np.sin(angle)
    sin[:, 0] = 1.0 - 2.0 * (long % 2)
    single = interleave(cos, sin)
    wide = np.stack([*split(pair), *split(single)])
    i = np.arange(LANES)
    angle = 2.0 * np.pi * (np.outer(i, i) % LANES) / LANES
    tall = np.stack(split(np.concatenate([np.cos(angle), np.sin(angle)], axis=1)))

    def turns(count, size):
        angle = 2.0 * np.pi * np.outer(np.arange(count), np.arange(size)) / TOTAL
        return np.stack([np.cos(angle), np.sin(angle)]).astype(np.float32)

    return wide, tall, turns(COLS // 2, WIDE), turns(ROWS, LANES)


SEND1, SEND2, SEND3, SEND4, SEND5, SEND6 = 0, 1, 4, 7, 9, 11


def kernel(
    u_hbm, v_hbm, wide_hbm, tall_hbm, turn1_hbm, turn2_hbm, s_out, a_out,
    fields, wide, tall, turn1, turn2, tables,
    got1, put2, got2, put3, got3, tiles, products, filtered, extra,
    put4, got4, put5, got5, put6, local_sem, send_sem, recv_sem,
):
    row, col = lax.axis_index("row"), lax.axis_index("col")
    mesh_id = pl.DeviceIdType.MESH

    loads = [
        pltpu.make_async_copy(src, dst, local_sem.at[n])
        for n, (src, dst) in enumerate(
            [
                (u_hbm, fields.at[0]),
                (v_hbm, fields.at[1]),
                (wide_hbm, wide),
                (tall_hbm, tall),
                (turn1_hbm, turn1),
                (turn2_hbm, turn2),
            ]
        )
    ]
    for load in loads:
        load.start()

    barrier = pltpu.get_barrier_semaphore()

    def greet(axis, me, size):
        def body(k, carry):
            pl.semaphore_signal(
                barrier, inc=1, device_id={axis: lax.rem(me + k, size)}, device_id_type=mesh_id
            )
            return carry

        lax.fori_loop(1, size, body, 0)

    greet("col", col, COLS)
    greet("row", row, ROWS)

    def send(axis, me, size, source, target, sem):
        def body(k, carry):
            peer = lax.rem(me + k, size)
            pltpu.make_async_remote_copy(
                src_ref=source(peer),
                dst_ref=target(me),
                send_sem=send_sem.at[sem],
                recv_sem=recv_sem.at[sem],
                device_id={axis: peer},
                device_id_type=mesh_id,
            ).start()
            return carry

        lax.fori_loop(1, size, body, 0)

    def whole(axis, me, size, block, sem):
        return pltpu.make_async_remote_copy(
            src_ref=block,
            dst_ref=block,
            send_sem=send_sem.at[sem],
            recv_sem=recv_sem.at[sem],
            device_id={axis: lax.rem(me + 1, size)},
            device_id_type=mesh_id,
        )

    pending = []

    def arrived(axis, me, size, block, sem):
        whole(axis, me, size, block, sem).wait_recv()

    def fill(step, carry):
        for n, table in enumerate(factors(step, row, col)):
            tables[n, step] = table
        return carry

    lax.fori_loop(0, ROWS, fill, 0)

    loads[0].wait()
    loads[1].wait()
    pl.semaphore_wait(barrier, COLS - 1 + ROWS - 1)

    send("col", col, COLS, lambda c: fields.at[:, c], lambda c: got1.at[c], SEND1)
    pending.append(("col", col, COLS, got1.at[pl.ds(0, COLS - 1)], SEND1))
    got1[col] = fields[:, col]
    for load in loads[2:]:
        load.wait()
    arrived("col", col, COLS, got1.at[pl.ds(0, COLS - 1)], SEND1)

    for n in range(3):
        if n < 2:
            values = [got1[c, n] for c in range(COLS)]
        else:
            values = [got1[c, 0] * got1[c, 1] * got1[c, 1] for c in range(COLS)]
        weights = [wide.at[k][...] for k in range(4)]
        blocks = forward_columns(values, turn1[0], turn1[1], weights)
        for c in range(COLS):
            put2[n, c] = blocks[c]
        send("col", col, COLS, lambda c: put2.at[n, c], lambda c: got2.at[n, c], SEND2 + n)
        pending.append(("col", col, COLS, put2.at[n, pl.ds(0, COLS - 1)], SEND2 + n))
        got2[n, col] = put2[n, col]

    for n in range(3):
        arrived("col", col, COLS, got2.at[n, pl.ds(0, COLS - 1)], SEND2 + n)
        block = got2[n].reshape(COLS * 8, WIDE)
        put3[n] = block.T.reshape(ROWS, 8, LANES)
        send("row", row, ROWS, lambda r: put3.at[n, r], lambda r: got3.at[n, r], SEND3 + n)
        pending.append(("row", row, ROWS, put3.at[n, pl.ds(0, ROWS - 1)], SEND3 + n))
        got3[n, row] = put3[n, row]

    sign = part_sign()
    for n in range(3):
        arrived("row", row, ROWS, got3.at[n, pl.ds(0, ROWS - 1)], SEND3 + n)
        spectrum = tile_fft([got3[n, r] for r in range(ROWS)], sign, -1)
        for k in range(ROWS):
            cosine, sine = turn2[0, k : k + 1, :], turn2[1, k : k + 1, :]
            tiles[k] = tile_turn(spectrum[k], sign, cosine, -sine)
        out = dot3(tiles[...].reshape(ROWS * 8, LANES), tall[0], tall[1], FORWARD)
        products[n] = out.reshape(ROWS, 8, 2 * LANES)

    def filter_step(k, carry):
        spectra = []
        for n in range(3):
            both = products[n, k]
            spectra.append(both[:, :LANES] + sign * roll_rows(both[:, LANES:], 4))
        for n, tile in enumerate(advance(*spectra, [tables[m, k] for m in range(6)])):
            filtered[n, k] = tile
        return carry

    lax.fori_loop(0, ROWS, filter_step, 0)

    special = sublane() == jnp.where(row + col == 0, 4, -1)
    for n in (2, 0, 1):
        block = filtered[n].reshape(ROWS * 8, LANES)
        products[n] = dot3(block, tall[0], tall[1], FORWARD).reshape(ROWS, 8, 2 * LANES)
        turned = []
        for k in range(ROWS):
            both = products[n, k]
            tile = both[:, :LANES] - sign * roll_rows(both[:, LANES:], 4)
            cosine, sine = turn2[0, k : k + 1, :], turn2[1, k : k + 1, :]
            turned.append(tile_turn(tile, sign, cosine, sine))
        values = tile_fft(turned, sign, 1)
        for r in range(ROWS):
            if n == 2:
                extra[r] = values[r]
            elif n == 0:
                put4[n, r] = jnp.where(special, extra[r], values[r])
            else:
                put4[n, r] = jnp.where(special, roll_rows(extra[r], 7), values[r])
        if n == 2:
            continue
        send("row", row, ROWS, lambda r: put4.at[n, r], lambda r: got4.at[n, r], SEND4 + n)
        pending.append(("row", row, ROWS, put4.at[n, pl.ds(0, ROWS - 1)], SEND4 + n))
        got4[n, row] = put4[n, row]

    for n in range(2):
        arrived("row", row, ROWS, got4.at[n, pl.ds(0, ROWS - 1)], SEND4 + n)
        block = got4[n].reshape(ROWS * 8, LANES)
        put5[n] = block.T.reshape(COLS, 8, WIDE)
        send("col", col, COLS, lambda c: put5.at[n, c], lambda c: got5.at[n, c], SEND5 + n)
        pending.append(("col", col, COLS, put5.at[n, pl.ds(0, COLS - 1)], SEND5 + n))
        got5[n, col] = put5[n, col]

    _, feed = growth_forcing_at_zero()
    last = []
    for n, out in enumerate((s_out, a_out)):
        arrived("col", col, COLS, got5.at[n, pl.ds(0, COLS - 1)], SEND5 + n)
        weights = [wide.at[k][...] for k in range(4)]
        values = backward_columns([got5[n, c] for c in range(COLS)], turn1[0], turn1[1], weights)
        for c in range(COLS):
            put6[n, c] = values[c] + feed if n == 0 else values[c]
        send("col", col, COLS, lambda c: put6.at[n, c], lambda c: out.at[c], SEND6 + n)
        pending.append(("col", col, COLS, put6.at[n, pl.ds(0, COLS - 1)], SEND6 + n))
        own = pltpu.make_async_copy(put6.at[n, col], out.at[col], local_sem.at[n])
        own.start()
        last.append(own)

    for n, out in enumerate((s_out, a_out)):
        arrived("col", col, COLS, out.at[pl.ds(0, COLS - 1)], SEND6 + n)
        last[n].wait()
    for entry in pending:
        whole(*entry).wait_send()


def growth_forcing_at_zero():
    linear = -FEED_RATE
    return math.exp(HALF_STEP * linear), FEED_RATE * math.expm1(HALF_STEP * linear) / linear


def on_device(substrate, activator):
    wide, tall, turn1, turn2 = constants()
    shape = jax.ShapeDtypeStruct((COLS, 8, WIDE), F32)
    anywhere = pl.BlockSpec(memory_space=pl.ANY)
    vmem = lambda *shape: pltpu.VMEM(shape, F32)
    by_col, by_row = (COLS, 8, WIDE), (ROWS, 8, LANES)
    out = pl.pallas_call(
        kernel,
        name="section",
        out_shape=(shape, shape),
        in_specs=[anywhere] * 6,
        out_specs=(anywhere, anywhere),
        scratch_shapes=[
            vmem(2, *by_col),
            pltpu.VMEM(wide.shape, BF16),
            pltpu.VMEM(tall.shape, BF16),
            vmem(*turn1.shape),
            vmem(*turn2.shape),
            vmem(6, *by_row),
            vmem(COLS, 2, 8, WIDE),
            vmem(3, *by_col),
            vmem(3, *by_col),
            vmem(3, *by_row),
            vmem(3, *by_row),
            vmem(*by_row),
            vmem(3, ROWS, 8, 2 * LANES),
            vmem(3, *by_row),
            vmem(*by_row),
            vmem(2, *by_row),
            vmem(2, *by_row),
            vmem(2, *by_col),
            vmem(2, *by_col),
            vmem(2, *by_col),
            pltpu.SemaphoreType.DMA((6,)),
            pltpu.SemaphoreType.DMA((13,)),
            pltpu.SemaphoreType.DMA((13,)),
        ],
        compiler_params=pltpu.CompilerParams(collective_id=0, has_side_effects=True),
    )(
        substrate.reshape(COLS, 8, WIDE),
        activator.reshape(COLS, 8, WIDE),
        wide,
        tall,
        turn1,
        turn2,
    )
    return tuple(x.reshape(substrate.shape) for x in out)


def solution(mesh):
    spec = P("row", "col")
    return jax.shard_map(
        on_device, mesh=mesh, in_specs=(spec, spec), out_specs=(spec, spec), check_vma=False
    )
```

```python
import math

import jax
import jax.numpy as jnp
import numpy as np
from jax import lax
from jax.experimental import pallas as pl
from jax.experimental.pallas import tpu as pltpu
from jax.sharding import PartitionSpec as P

FEED_RATE = 0.037
KILL_RATE = 0.06
HALF_STEP = 4.0
SUBSTRATE = (4e-07, FEED_RATE)
ACTIVATOR = (2e-07, FEED_RATE + KILL_RATE)
TOTAL = 4096
COLS = 16
ROWS = 32
WIDE = 256
LANES = 128
F32 = jnp.float32
BF16 = jnp.bfloat16


def c_add(a, b):
    im = a[1] if b[1] is None else (b[1] if a[1] is None else a[1] + b[1])
    return (a[0] + b[0], im)


def c_sub(a, b):
    im = a[1] if b[1] is None else (-b[1] if a[1] is None else a[1] - b[1])
    return (a[0] - b[0], im)


def c_conj(a):
    return (a[0], None if a[1] is None else -a[1])


def c_turn(a, numerator, denominator):
    numerator %= denominator
    if numerator == 0:
        return a
    if 4 * numerator == denominator:
        return (jnp.zeros_like(a[0]) if a[1] is None else -a[1], a[0])
    if 4 * numerator == 3 * denominator:
        return (jnp.zeros_like(a[0]) if a[1] is None else a[1], -a[0])
    cosine = math.cos(2.0 * math.pi * numerator / denominator)
    sine = math.sin(2.0 * math.pi * numerator / denominator)
    if a[1] is None:
        return (a[0] * cosine, a[0] * sine)
    return (a[0] * cosine - a[1] * sine, a[0] * sine + a[1] * cosine)


def real_forward(values):
    size = len(values)
    if size == 2:
        return [(values[0] + values[1], None), (values[0] - values[1], None)]
    even, odd = real_forward(values[::2]), real_forward(values[1::2])
    return join_halves(even, odd, size)


def join_halves(even, odd, size, first=0):
    half = size // 2
    out = [None] * (half + 1)
    for k in range(first, half // 2 + 1):
        turned = c_turn(odd[k], -k, size)
        out[k] = c_add(even[k], turned)
        if half - k != k:
            out[half - k] = c_conj(c_sub(even[k], turned))
    return out


def split_halves(spectrum, size, first=0):
    half = size // 2
    even, odd = [None] * (half // 2 + 1), [None] * (half // 2 + 1)
    for k in range(first, half // 2 + 1):
        if k == 0:
            even[k] = (spectrum[0][0] + spectrum[half][0], None)
            odd[k] = (spectrum[0][0] - spectrum[half][0], None)
        elif 2 * k == half:
            even[k] = (2.0 * spectrum[k][0], None)
            odd[k] = (-2.0 * spectrum[k][1], None)
        else:
            other = c_conj(spectrum[half - k])
            even[k] = c_add(spectrum[k], other)
            odd[k] = c_turn(c_sub(spectrum[k], other), k, size)
    return even, odd


def real_backward(spectrum):
    size = 2 * (len(spectrum) - 1)
    if size == 2:
        a, b = spectrum[0][0], spectrum[1][0]
        return [a + b, a - b]
    even, odd = split_halves(spectrum, size)
    even, odd = real_backward(even), real_backward(odd)
    return [x for pair in zip(even, odd) for x in pair]


def roll_rows(tile, shift):
    return pltpu.roll(tile, shift, 0)


def sublane():
    return lax.broadcasted_iota(jnp.int32, (8, LANES), 0)


def part_sign():
    return jnp.where(sublane() < 4, 1.0, -1.0).astype(F32)


def tile_turn(tile, sign, cosine, sine):
    return tile * cosine - (sign * sine) * roll_rows(tile, 4)


def tile_fft(tiles, sign, direction):
    size = len(tiles)
    if size == 1:
        return tiles
    even, odd = tile_fft(tiles[::2], sign, direction), tile_fft(tiles[1::2], sign, direction)
    low, high = [], []
    for k in range(size // 2):
        turned = odd[k]
        if 4 * k == size:
            turned = (-direction * sign) * roll_rows(turned, 4)
        elif k:
            angle = direction * 2.0 * math.pi * k / size
            turned = tile_turn(turned, sign, math.cos(angle), math.sin(angle))
        low.append(even[k] + turned)
        high.append(even[k] - turned)
    return low + high


def dot3(values, high, low, dims):
    dot = lambda a, b: lax.dot_general(a, b, (dims, ((), ())), preferred_element_type=F32)
    top = values.astype(BF16)
    rest = (values - top.astype(F32)).astype(BF16)
    return dot(top, high) + (dot(rest, high) + dot(top, low))


FORWARD = ((1,), (0,))


def forward_columns(values, turn_cos, turn_sin, weights):
    even, odd = real_forward(values[::2]), real_forward(values[1::2])
    spectrum = join_halves(even, odd, COLS, 1)
    rows = [jnp.concatenate([even[0][0], odd[0][0]], axis=1)]
    for k in range(1, COLS // 2):
        re, im = spectrum[k]
        cosine, sine = turn_cos[k : k + 1, :], turn_sin[k : k + 1, :]
        rows.append(jnp.concatenate([re * cosine + im * sine, im * cosine - re * sine], axis=1))
    stacked = jnp.concatenate(rows, axis=0)
    out = dot3(stacked, weights[0], weights[1], FORWARD)
    first = dot3(stacked[:16], weights[2], weights[3], FORWARD)
    blocks = []
    for slot in range(COLS // 2):
        row = first[:8] if slot == 0 else out[8 * slot : 8 * slot + 8]
        blocks += [row[:, :WIDE], row[:, WIDE:]]
    return blocks


def backward_columns(blocks, turn_cos, turn_sin, weights):
    stacked = jnp.concatenate(
        [jnp.concatenate([blocks[2 * s], blocks[2 * s + 1]], axis=1) for s in range(COLS // 2)],
        axis=0,
    )
    out = dot3(stacked, weights[0], weights[1], FORWARD)
    first = dot3(stacked[:16], weights[2], weights[3], FORWARD)
    spectrum = [None] * (COLS // 2)
    for k in range(1, COLS // 2):
        row = out[8 * k : 8 * k + 8]
        re, im = row[:, :WIDE], row[:, WIDE:]
        cosine, sine = turn_cos[k : k + 1, :], turn_sin[k : k + 1, :]
        spectrum[k] = (re * cosine - im * sine, im * cosine + re * sine)
    even, odd = split_halves(spectrum + [None], COLS, 1)
    even[0], odd[0] = (first[:8, :WIDE], None), (first[:8, WIDE:], None)
    even, odd = real_backward(even), real_backward(odd)
    return [x for pair in zip(even, odd) for x in pair]


def squared_wave(index):
    signed = jnp.where(2 * index < TOTAL, index, index - TOTAL).astype(F32)
    angular = (2.0 * math.pi) * signed
    return angular * angular


def growth_forcing(wave_number, diffusion, decay_rate):
    linear = -diffusion * wave_number - decay_rate
    growth = jnp.exp(HALF_STEP * linear)
    return growth, (growth - 1.0) / linear


def factors(step, row, col):
    column = sublane() % 4
    slot, half = col // 2, col % 2
    within = LANES * half + 4 * row + column
    q = jnp.where(slot == 0, 8 * within, slot + COLS * within)
    p = step + ROWS * lax.broadcasted_iota(jnp.int32, (8, LANES), 1)
    row_wave = squared_wave(p)
    wave_number = row_wave + squared_wave(q)
    last = row_wave + (2.0 * math.pi * (TOTAL // 2)) ** 2
    norm = 1.0 / (TOTAL * TOTAL)
    paired = jnp.where(q == 0, 1.0, jnp.where(slot == 0, 2.0, 1.0)).astype(F32)
    out = []
    for species, sign in ((SUBSTRATE, -1.0), (ACTIVATOR, 1.0)):
        for waves, scale in ((wave_number, paired * norm), (last, norm)):
            growth, forcing = growth_forcing(waves, *species)
            out += [growth * scale, forcing * (scale * sign)]
    return out


def constants():
    def split(matrix):
        high = matrix.astype(np.float32).astype(BF16)
        return high, (matrix - high.astype(np.float64)).astype(np.float32).astype(BF16)

    def interleave(re, im):
        size = re.shape[0]
        return np.stack([re.reshape(size, -1, 4), im.reshape(size, -1, 4)], axis=2).reshape(size, -1)

    j = np.arange(WIDE)
    angle = 2.0 * np.pi * (np.outer(j, j) % WIDE) / WIDE
    cos, sin = np.cos(angle), np.sin(angle)
    pair = interleave(np.concatenate([cos, sin]), np.concatenate([-sin, cos]))
    long = np.arange(2 * WIDE)
    angle = 2.0 * np.pi * (np.outer(long, j) % (2 * WIDE)) / (2 * WIDE)
    cos, sin = np.cos(angle), -np.sin(angle)
    sin[:, 0] = 1.0 - 2.0 * (long % 2)
    single = interleave(cos, sin)
    wide = np.stack([*split(pair), *split(single)])
    i = np.arange(LANES)
    angle = 2.0 * np.pi * (np.outer(i, i) % LANES) / LANES
    tall = np.stack(split(np.concatenate([np.cos(angle), np.sin(angle)], axis=1)))

    def turns(count, size):
        angle = 2.0 * np.pi * np.outer(np.arange(count), np.arange(size)) / TOTAL
        return np.stack([np.cos(angle), np.sin(angle)]).astype(np.float32)

    return wide, tall, turns(COLS // 2, WIDE), turns(ROWS, LANES)


SEND1, SEND2, SEND3, SEND4, SEND5, SEND6 = 0, 2, 5, 8, 10, 12
U, R, V = 0, 1, 2


def kernel(
    u_hbm, v_hbm, wide_hbm, tall_hbm, turn1_hbm, turn2_hbm, s_out, a_out,
    fields, wide, tall, turn1, turn2, tables, back,
    got1, put2, got2, put3, got3, tiles, spectra, pair, products,
    put4, got4, put5, got5, put6, local_sem, send_sem, recv_sem,
):
    row, col = lax.axis_index("row"), lax.axis_index("col")
    mesh_id = pl.DeviceIdType.MESH

    loads = [
        pltpu.make_async_copy(src, dst, local_sem.at[n])
        for n, (src, dst) in enumerate(
            [
                (u_hbm, fields.at[0]),
                (v_hbm, fields.at[1]),
                (wide_hbm, wide),
                (tall_hbm, tall),
                (turn1_hbm, turn1),
                (turn2_hbm, turn2),
            ]
        )
    ]
    for load in loads:
        load.start()

    barrier = pltpu.get_barrier_semaphore()

    def greet(axis, me, size):
        def body(k, carry):
            pl.semaphore_signal(
                barrier, inc=1, device_id={axis: lax.rem(me + k, size)}, device_id_type=mesh_id
            )
            return carry

        lax.fori_loop(1, size, body, 0)

    pending = []

    def piece(axis, peer, source, target, sem):
        return pltpu.make_async_remote_copy(
            src_ref=source,
            dst_ref=target,
            send_sem=send_sem.at[sem],
            recv_sem=recv_sem.at[sem],
            device_id={axis: peer},
            device_id_type=mesh_id,
        )

    def send(axis, source, target, sem):
        me, size = (col, COLS) if axis == "col" else (row, ROWS)

        def body(k, carry):
            peer = lax.rem(me + k, size)
            piece(axis, peer, source.at[peer], target.at[me], sem).start()
            return carry

        lax.fori_loop(1, size, body, 0)
        pending.append((axis, source, sem))

    def whole(axis, block, sem):
        me, size = (col, COLS) if axis == "col" else (row, ROWS)
        block = block.at[pl.ds(0, size - 1)]
        return piece(axis, lax.rem(me + 1, size), block, block, sem)

    greet("col", col, COLS)
    greet("row", row, ROWS)
    loads[0].wait()
    loads[1].wait()
    pl.semaphore_wait(barrier, COLS - 1 + ROWS - 1)

    for n in range(2):
        send("col", fields.at[n], got1.at[n], SEND1 + n)
        got1[n, col] = fields[n, col]

    def fill(step, carry):
        for n, table in enumerate(factors(step, row, col)):
            tables[n, step] = table
        return carry

    lax.fori_loop(0, ROWS, fill, 0)

    def forward_rows(n, values):
        blocks = forward_columns(
            values, turn1[0], turn1[1], [wide.at[k][...] for k in range(4)]
        )
        for c in range(COLS):
            put2[n, c] = blocks[c]
        send("col", put2.at[n], got2.at[n], SEND2 + n)
        got2[n, col] = put2[n, col]

    for load in loads[2:]:
        load.wait()
    whole("col", got1.at[0], SEND1).wait_recv()
    forward_rows(U, [got1[0, c] for c in range(COLS)])
    whole("col", got1.at[1], SEND1 + 1).wait_recv()
    forward_rows(R, [got1[0, c] * got1[1, c] * got1[1, c] for c in range(COLS)])
    forward_rows(V, [got1[1, c] for c in range(COLS)])

    for n in (U, R, V):
        whole("col", got2.at[n], SEND2 + n).wait_recv()
        block = got2[n].reshape(COLS * 8, WIDE)
        put3[n] = block.T.reshape(ROWS, 8, LANES)
        send("row", put3.at[n], got3.at[n], SEND3 + n)
        got3[n, row] = put3[n, row]

    sign = part_sign()

    def forward_down(n):
        whole("row", got3.at[n], SEND3 + n).wait_recv()
        values = tile_fft([got3[n, r] for r in range(ROWS)], sign, -1)
        for k in range(ROWS):
            cosine, sine = turn2[0, k : k + 1, :], turn2[1, k : k + 1, :]
            tiles[k] = tile_turn(values[k], sign, cosine, -sine)
        out = dot3(tiles[...].reshape(ROWS * 8, LANES), tall[0], tall[1], FORWARD)
        products[pl.ds(0, ROWS)] = out.reshape(ROWS, 8, 2 * LANES)
        for k in range(ROWS):
            both = products[k]
            spectra[n, k] = both[:, :LANES] + sign * roll_rows(both[:, LANES:], 4)

    special = sublane() == jnp.where(row + col == 0, 4, -1)

    def backward_down(n, field):
        for k in range(ROWS):
            own, source = spectra[field, k], spectra[R, k]
            for m in range(2):
                t = 4 * n + 2 * m
                pair[m * ROWS + k] = tables[t, k] * own + tables[t + 1, k] * source
        block = pair[...].reshape(2 * ROWS * 8, LANES)
        products[...] = dot3(block, tall[0], tall[1], FORWARD).reshape(2 * ROWS, 8, 2 * LANES)
        for m in (1, 0):
            turned = []
            for k in range(ROWS):
                both = products[m * ROWS + k]
                tile = both[:, :LANES] - sign * roll_rows(both[:, LANES:], 4)
                cosine, sine = turn2[0, k : k + 1, :], turn2[1, k : k + 1, :]
                turned.append(tile_turn(tile, sign, cosine, sine))
            values = tile_fft(turned, sign, 1)
            for r in range(ROWS):
                if m == 1:
                    tiles[r] = values[r]
                else:
                    put4[n, r] = jnp.where(special, tiles[r], values[r])
        send("row", put4.at[n], got4.at[n], SEND4 + n)
        got4[n, row] = put4[n, row]

    forward_down(U)
    forward_down(R)
    backward_down(0, U)
    forward_down(V)
    backward_down(1, V)

    for k in range(4):
        back[k] = wide.at[k][...].T

    for n in range(2):
        whole("row", got4.at[n], SEND4 + n).wait_recv()
        block = got4[n].reshape(ROWS * 8, LANES)
        put5[n] = block.T.reshape(COLS, 8, WIDE)
        send("col", put5.at[n], got5.at[n], SEND5 + n)
        got5[n, col] = put5[n, col]

    _, feed = growth_forcing_at_zero()
    for n, out in enumerate((s_out, a_out)):
        whole("col", got5.at[n], SEND5 + n).wait_recv()
        weights = [back.at[k][...] for k in range(4)]
        values = backward_columns([got5[n, c] for c in range(COLS)], turn1[0], turn1[1], weights)
        for c in range(COLS):
            put6[n, c] = values[c] + feed if n == 0 else values[c]
        send("col", put6.at[n], out, SEND6 + n)
        out[col] = put6[n, col]

    for n, out in enumerate((s_out, a_out)):
        whole("col", out, SEND6 + n).wait_recv()
    for entry in pending:
        whole(*entry).wait_send()


def growth_forcing_at_zero():
    linear = -FEED_RATE
    return math.exp(HALF_STEP * linear), FEED_RATE * math.expm1(HALF_STEP * linear) / linear


def on_device(substrate, activator):
    wide, tall, turn1, turn2 = constants()
    shape = pltpu.VMEM((COLS, 8, WIDE), F32)
    held = lambda x: pltpu.with_memory_space_constraint(x, pltpu.HBM)
    anywhere = pl.BlockSpec(memory_space=pltpu.HBM)
    vmem = lambda *shape: pltpu.VMEM(shape, F32)
    by_col, by_row = (COLS, 8, WIDE), (ROWS, 8, LANES)
    out = pl.pallas_call(
        kernel,
        name="section",
        out_shape=(shape, shape),
        in_specs=[anywhere] * 6,
        out_specs=(pl.BlockSpec(memory_space=pltpu.VMEM),) * 2,
        scratch_shapes=[
            vmem(2, *by_col),
            pltpu.VMEM(wide.shape, BF16),
            pltpu.VMEM(tall.shape, BF16),
            vmem(*turn1.shape),
            vmem(*turn2.shape),
            vmem(8, *by_row),
            pltpu.VMEM(wide.shape, BF16),
            vmem(2, *by_col),
            vmem(3, *by_col),
            vmem(3, *by_col),
            vmem(3, *by_row),
            vmem(3, *by_row),
            vmem(*by_row),
            vmem(3, *by_row),
            vmem(2 * ROWS, 8, LANES),
            vmem(2 * ROWS, 8, 2 * LANES),
            vmem(2, *by_row),
            vmem(2, *by_row),
            vmem(2, *by_col),
            vmem(2, *by_col),
            vmem(2, *by_col),
            pltpu.SemaphoreType.DMA((6,)),
            pltpu.SemaphoreType.DMA((14,)),
            pltpu.SemaphoreType.DMA((14,)),
        ],
        compiler_params=pltpu.CompilerParams(
            collective_id=0, has_side_effects=True, vmem_limit_bytes=20 << 20
        ),
    )(
        held(substrate.reshape(COLS, 8, WIDE)),
        held(activator.reshape(COLS, 8, WIDE)),
        held(jnp.asarray(wide)),
        held(jnp.asarray(tall)),
        held(jnp.asarray(turn1)),
        held(jnp.asarray(turn2)),
    )
    return tuple(x.reshape(substrate.shape) for x in out)


def solution(mesh):
    spec = P("row", "col")
    return jax.shard_map(
        on_device, mesh=mesh, in_specs=(spec, spec), out_specs=(spec, spec), check_vma=False
    )
```

```python
import math

import jax
import jax.numpy as jnp
import numpy as np
from jax import lax
from jax.experimental import pallas as pl
from jax.experimental.pallas import tpu as pltpu
from jax.sharding import PartitionSpec as P

FEED_RATE = 0.037
KILL_RATE = 0.06
HALF_STEP = 4.0
SUBSTRATE = (4e-07, FEED_RATE)
ACTIVATOR = (2e-07, FEED_RATE + KILL_RATE)
TOTAL = 4096
COLS = 16
ROWS = 32
WIDE = 256
LANES = 128
TILES = ROWS // 2
F32 = jnp.float32
BF16 = jnp.bfloat16


def c_add(a, b):
    im = a[1] if b[1] is None else (b[1] if a[1] is None else a[1] + b[1])
    return (a[0] + b[0], im)


def c_sub(a, b):
    im = a[1] if b[1] is None else (-b[1] if a[1] is None else a[1] - b[1])
    return (a[0] - b[0], im)


def c_conj(a):
    return (a[0], None if a[1] is None else -a[1])


def c_turn(a, numerator, denominator):
    numerator %= denominator
    if numerator == 0:
        return a
    if 4 * numerator == denominator:
        return (jnp.zeros_like(a[0]) if a[1] is None else -a[1], a[0])
    if 4 * numerator == 3 * denominator:
        return (jnp.zeros_like(a[0]) if a[1] is None else a[1], -a[0])
    cosine = math.cos(2.0 * math.pi * numerator / denominator)
    sine = math.sin(2.0 * math.pi * numerator / denominator)
    if a[1] is None:
        return (a[0] * cosine, a[0] * sine)
    return (a[0] * cosine - a[1] * sine, a[0] * sine + a[1] * cosine)


def real_forward(values):
    size = len(values)
    if size == 2:
        return [(values[0] + values[1], None), (values[0] - values[1], None)]
    even, odd = real_forward(values[::2]), real_forward(values[1::2])
    return join_halves(even, odd, size)


def join_halves(even, odd, size, first=0):
    half = size // 2
    out = [None] * (half + 1)
    for k in range(first, half // 2 + 1):
        turned = c_turn(odd[k], -k, size)
        out[k] = c_add(even[k], turned)
        if half - k != k:
            out[half - k] = c_conj(c_sub(even[k], turned))
    return out


def split_halves(spectrum, size, first=0):
    half = size // 2
    even, odd = [None] * (half // 2 + 1), [None] * (half // 2 + 1)
    for k in range(first, half // 2 + 1):
        if k == 0:
            even[k] = (spectrum[0][0] + spectrum[half][0], None)
            odd[k] = (spectrum[0][0] - spectrum[half][0], None)
        elif 2 * k == half:
            even[k] = (2.0 * spectrum[k][0], None)
            odd[k] = (-2.0 * spectrum[k][1], None)
        else:
            other = c_conj(spectrum[half - k])
            even[k] = c_add(spectrum[k], other)
            odd[k] = c_turn(c_sub(spectrum[k], other), k, size)
    return even, odd


def real_backward(spectrum):
    size = 2 * (len(spectrum) - 1)
    if size == 2:
        a, b = spectrum[0][0], spectrum[1][0]
        return [a + b, a - b]
    even, odd = split_halves(spectrum, size)
    even, odd = real_backward(even), real_backward(odd)
    return [x for pair in zip(even, odd) for x in pair]


def roll_rows(tile, shift):
    return pltpu.roll(tile, shift, 0)


def sublane():
    return lax.broadcasted_iota(jnp.int32, (8, LANES), 0)


def part_sign():
    return jnp.where(sublane() % 4 < 2, 1.0, -1.0).astype(F32)


def other_part(tile):
    return jnp.where(sublane() % 4 < 2, roll_rows(tile, 6), roll_rows(tile, 2))


def tile_turn(tile, cosine, signed_sine):
    return tile * cosine - signed_sine * other_part(tile)


def tile_fft(tiles, sign, direction):
    size = len(tiles)
    if size == 1:
        return tiles
    even, odd = tile_fft(tiles[::2], sign, direction), tile_fft(tiles[1::2], sign, direction)
    low, high = [], []
    for k in range(size // 2):
        turned = odd[k]
        if 4 * k == size:
            turned = (-direction * sign) * other_part(turned)
        elif k:
            angle = direction * 2.0 * math.pi * k / size
            turned = tile_turn(turned, math.cos(angle), sign * math.sin(angle))
        low.append(even[k] + turned)
        high.append(even[k] - turned)
    return low + high


def second_turn(tile, k, sign, direction):
    if k == 0:
        return tile
    angle = direction * 2.0 * math.pi * k / ROWS
    lower = sublane() < 4
    cosine = jnp.where(lower, 1.0, math.cos(angle)).astype(F32)
    sine = jnp.where(lower, 0.0, math.sin(angle)).astype(F32)
    return tile_turn(tile, cosine, sign * sine)


def block_sums(tile):
    return jnp.where(sublane() < 4, tile, -tile) + roll_rows(tile, 4)


def fft_down(tiles, sign):
    turned = [second_turn(x, k, sign, -1) for k, x in enumerate(tile_fft(tiles, sign, -1))]
    return [block_sums(x) for x in turned]


def fft_up(tiles, sign):
    turned = [second_turn(block_sums(x), k, sign, 1) for k, x in enumerate(tiles)]
    return tile_fft(turned, sign, 1)


MATRIX = (((1,), (0,)), ((), ()))


def pieces(values):
    top = values.astype(BF16)
    return top, (values - top.astype(F32)).astype(BF16)


def dot_wide(values, high, low):
    top, rest = pieces(values)
    size = values.shape[0]
    both = lax.dot_general(
        jnp.concatenate([top, rest], axis=0), high, MATRIX, preferred_element_type=F32
    )
    corner = lax.dot_general(top, low, MATRIX, preferred_element_type=F32)
    return both[:size] + (both[size:] + corner)


def dot_tall(values, matrix):
    top, rest = pieces(values)
    return lax.dot_general(
        jnp.concatenate([top, rest, top], axis=1), matrix, MATRIX, preferred_element_type=F32
    )


def forward_columns(values, turn_cos, turn_sin, weights):
    even, odd = real_forward(values[::2]), real_forward(values[1::2])
    spectrum = join_halves(even, odd, COLS, 1)
    rows = [jnp.concatenate([even[0][0], odd[0][0]], axis=1)]
    for k in range(1, COLS // 2):
        re, im = spectrum[k]
        cosine, sine = turn_cos[k : k + 1, :], turn_sin[k : k + 1, :]
        rows.append(jnp.concatenate([re * cosine + im * sine, im * cosine - re * sine], axis=1))
    stacked = jnp.concatenate(rows, axis=0)
    out = dot_wide(stacked, weights[0], weights[1])
    first = dot_wide(stacked[:16], weights[2], weights[3])
    blocks = [[], []]
    for slot in range(COLS // 2):
        row = first[:8] if slot == 0 else out[8 * slot : 8 * slot + 8]
        for n in range(4):
            blocks[n % 2].append(row[:, LANES * n : LANES * (n + 1)])
    return blocks


def backward_columns(blocks, turn_cos, turn_sin, weights):
    rows = []
    for s in range(COLS // 2):
        row = [blocks[0][2 * s], blocks[1][2 * s], blocks[0][2 * s + 1], blocks[1][2 * s + 1]]
        rows.append(jnp.concatenate(row, axis=1))
    stacked = jnp.concatenate(rows, axis=0)
    out = dot_wide(stacked, weights[0], weights[1])
    first = dot_wide(stacked[:16], weights[2], weights[3])
    spectrum = [None] * (COLS // 2)
    for k in range(1, COLS // 2):
        row = out[8 * k : 8 * k + 8]
        re, im = row[:, :WIDE], row[:, WIDE:]
        cosine, sine = turn_cos[k : k + 1, :], turn_sin[k : k + 1, :]
        spectrum[k] = (re * cosine - im * sine, im * cosine + re * sine)
    even, odd = split_halves(spectrum + [None], COLS, 1)
    even[0], odd[0] = (first[:8, :WIDE], None), (first[:8, WIDE:], None)
    even, odd = real_backward(even), real_backward(odd)
    return [x for pair in zip(even, odd) for x in pair]


def squared_wave(index):
    signed = jnp.where(2 * index < TOTAL, index, index - TOTAL).astype(F32)
    angular = (2.0 * math.pi) * signed
    return angular * angular


def growth_forcing(wave_number, diffusion, decay_rate):
    linear = -diffusion * wave_number - decay_rate
    growth = jnp.exp(HALF_STEP * linear)
    return growth, (growth - 1.0) / linear


def factors(step, half, row, col):
    column = 2 * half + sublane() % 2
    slot, side = col // 2, col % 2
    within = LANES * side + 4 * row + column
    q = jnp.where(slot == 0, 8 * within, slot + COLS * within)
    p = step + TILES * (sublane() // 4) + ROWS * lax.broadcasted_iota(jnp.int32, (8, LANES), 1)
    row_wave = squared_wave(p)
    wave_number = row_wave + squared_wave(q)
    last = row_wave + (2.0 * math.pi * (TOTAL // 2)) ** 2
    norm = 1.0 / (TOTAL * TOTAL)
    paired = jnp.where(q == 0, 1.0, jnp.where(slot == 0, 2.0, 1.0)).astype(F32)
    out = []
    for species, sign in ((SUBSTRATE, -1.0), (ACTIVATOR, 1.0)):
        for waves, scale in ((wave_number, paired * norm), (last, norm))[: 2 - half]:
            growth, forcing = growth_forcing(waves, *species)
            out += [growth * scale, forcing * (scale * sign)]
    return out


def constants():
    def split(matrix):
        high = matrix.astype(np.float32).astype(BF16)
        return high, (matrix - high.astype(np.float64)).astype(np.float32).astype(BF16)

    def interleave(re, im):
        both = np.stack([re, im], axis=1).reshape(-1, 2, 2, ROWS, 2, 2)
        return both.transpose(0, 2, 4, 3, 1, 5).reshape(re.shape[0], -1)

    j = np.arange(WIDE)
    angle = 2.0 * np.pi * (np.outer(j, j) % WIDE) / WIDE
    cos, sin = np.cos(angle), np.sin(angle)
    pair = interleave(np.concatenate([cos, sin]), np.concatenate([-sin, cos]))
    long = np.arange(2 * WIDE)
    angle = 2.0 * np.pi * (np.outer(long, j) % (2 * WIDE)) / (2 * WIDE)
    cos, sin = np.cos(angle), -np.sin(angle)
    sin[:, 0] = 1.0 - 2.0 * (long % 2)
    single = interleave(cos, sin)
    wide = np.stack([*split(pair), *split(single)])
    i = np.arange(LANES)
    angle = 2.0 * np.pi * (np.outer(i, i) % LANES) / LANES
    high, low = split(np.concatenate([np.cos(angle), np.sin(angle)], axis=1))
    tall = np.concatenate([high, high, low])

    angle = 2.0 * np.pi * np.outer(np.arange(COLS // 2), j) / TOTAL
    turn1 = np.stack([np.cos(angle), np.sin(angle)]).astype(np.float32)
    block, part, _ = np.unravel_index(np.arange(8), (2, 2, 2))
    wave = np.arange(TILES)[:, None] + TILES * block
    angle = 2.0 * np.pi * wave[:, :, None] * i / TOTAL
    sign = np.where(part == 0, 1.0, -1.0)[:, None]
    turn2 = np.stack([np.cos(angle), sign * np.sin(angle)]).astype(np.float32)
    return wide, tall, turn1, turn2


SEND1, SEND2, SEND3, SEND4, SEND5, SEND6 = 0, 2, 8, 14, 18, 22
U, R, V = 0, 1, 2


def kernel(
    u_hbm, v_hbm, wide_hbm, tall_hbm, turn1_hbm, turn2_hbm, s_out, a_out,
    fields, wide, tall, turn1, turn2, tables, back,
    got1, put2, got2, put3, got3, tiles, spectra, pair, products,
    put4, got4, put5, got5, put6, local_sem, send_sem, recv_sem,
):
    row, col = lax.axis_index("row"), lax.axis_index("col")
    mesh_id = pl.DeviceIdType.MESH

    loads = [
        pltpu.make_async_copy(src, dst, local_sem.at[n])
        for n, (src, dst) in enumerate(
            [
                (u_hbm, fields.at[0]),
                (v_hbm, fields.at[1]),
                (wide_hbm, wide),
                (tall_hbm, tall),
                (turn1_hbm, turn1),
                (turn2_hbm, turn2),
            ]
        )
    ]
    for load in loads:
        load.start()

    barrier = pltpu.get_barrier_semaphore()

    def greet(axis, me, size):
        def body(k, carry):
            pl.semaphore_signal(
                barrier, inc=1, device_id={axis: lax.rem(me + k, size)}, device_id_type=mesh_id
            )
            return carry

        lax.fori_loop(1, size, body, 0)

    pending = []

    def piece(axis, peer, source, target, sem):
        return pltpu.make_async_remote_copy(
            src_ref=source,
            dst_ref=target,
            send_sem=send_sem.at[sem],
            recv_sem=recv_sem.at[sem],
            device_id={axis: peer},
            device_id_type=mesh_id,
        )

    def send(axis, source, target, sem):
        me, size = (col, COLS) if axis == "col" else (row, ROWS)

        def body(k, carry):
            peer = lax.rem(me + k, size)
            piece(axis, peer, source.at[peer], target.at[me], sem).start()
            return carry

        lax.fori_loop(1, size, body, 0)
        pending.append((axis, source, sem))

    def whole(axis, block, sem):
        me, size = (col, COLS) if axis == "col" else (row, ROWS)
        block = block.at[pl.ds(0, size - 1)]
        return piece(axis, lax.rem(me + 1, size), block, block, sem)

    greet("col", col, COLS)
    greet("row", row, ROWS)
    loads[0].wait()
    pl.semaphore_wait(barrier, COLS - 1 + ROWS - 1)

    for n in range(2):
        if n == 1:
            loads[1].wait()
        send("col", fields.at[n], got1.at[n], SEND1 + n)
        got1[n, col] = fields[n, col]

    def fill(step, carry):
        for half in range(2):
            for n, table in enumerate(factors(step, half, row, col)):
                tables[8 * half + n, step] = table
        return carry

    lax.fori_loop(0, TILES, fill, 0)

    def forward_rows(n, values):
        blocks = forward_columns(
            values, turn1[0], turn1[1], [wide.at[k][...] for k in range(4)]
        )
        for h in range(2):
            for c in range(COLS):
                put2[n, h, c] = blocks[h][c]
            send("col", put2.at[n, h], got2.at[n, h], SEND2 + 2 * n + h)
            got2[n, h, col] = put2[n, h, col]

    for load in loads[2:]:
        load.wait()
    whole("col", got1.at[0], SEND1).wait_recv()
    forward_rows(U, [got1[0, c] for c in range(COLS)])
    whole("col", got1.at[1], SEND1 + 1).wait_recv()
    forward_rows(R, [got1[0, c] * got1[1, c] * got1[1, c] for c in range(COLS)])
    forward_rows(V, [got1[1, c] for c in range(COLS)])

    for n in (U, R, V):
        for h in range(2):
            whole("col", got2.at[n, h], SEND2 + 2 * n + h).wait_recv()
            turned = got2[n, h].reshape(LANES, LANES).T
            for r in range(ROWS):
                put3[n, h, r] = turned[4 * r : 4 * r + 4]
            send("row", put3.at[n, h], got3.at[n, h], SEND3 + 2 * n + h)
            got3[n, h, row] = put3[n, h, row]

    sign = part_sign()

    def two_blocks(ref, t):
        return jnp.concatenate([ref[2 * t], ref[2 * t + 1]], axis=0)

    def forward_down(n, h):
        whole("row", got3.at[n, h], SEND3 + 2 * n + h).wait_recv()
        values = fft_down([two_blocks(got3.at[n, h], t) for t in range(TILES)], sign)
        for k in range(TILES):
            tiles[k] = tile_turn(values[k], turn2[0, k], -turn2[1, k])
        out = dot_tall(tiles[...].reshape(LANES, LANES), tall[...])
        products[pl.ds(0, TILES)] = out.reshape(TILES, 8, 2 * LANES)
        for k in range(TILES):
            both = products[k]
            spectra[n, h, k] = both[:, :LANES] + sign * other_part(both[:, LANES:])

    special = sublane() % 4 == jnp.where(row + col == 0, 2, -1)

    def backward_down(n, field, h):
        parts = 2 - h
        for k in range(TILES):
            own, source = spectra[field, h, k], spectra[R, h, k]
            for m in range(parts):
                t = 8 * h + 2 * (parts * n + m)
                pair[m * TILES + k] = tables[t, k] * own + tables[t + 1, k] * source
        block = pair[pl.ds(0, parts * TILES)].reshape(parts * LANES, LANES)
        out = dot_tall(block, tall[...])
        products[pl.ds(0, parts * TILES)] = out.reshape(parts * TILES, 8, 2 * LANES)
        for m in reversed(range(parts)):
            turned = []
            for k in range(TILES):
                both = products[m * TILES + k]
                tile = both[:, :LANES] - sign * other_part(both[:, LANES:])
                turned.append(tile_turn(tile, turn2[0, k], turn2[1, k]))
            values = fft_up(turned, sign)
            for t in range(TILES):
                value = values[t]
                if m == 1:
                    tiles[t] = value
                    continue
                if h == 0:
                    value = jnp.where(special, tiles[t], value)
                put4[n, h, 2 * t] = value[:4]
                put4[n, h, 2 * t + 1] = value[4:]
        send("row", put4.at[n, h], got4.at[n, h], SEND4 + 2 * n + h)
        got4[n, h, row] = put4[n, h, row]

    forward_down(U, 0)
    forward_down(U, 1)
    for h in range(2):
        forward_down(R, h)
        backward_down(0, U, h)
    for h in range(2):
        forward_down(V, h)
        backward_down(1, V, h)

    for k in range(4):
        back[k] = wide.at[k][...].T

    for n in range(2):
        for h in range(2):
            whole("row", got4.at[n, h], SEND4 + 2 * n + h).wait_recv()
            block = jnp.concatenate([two_blocks(got4.at[n, h], t) for t in range(TILES)], axis=0)
            put5[n, h] = block.T.reshape(COLS, 8, LANES)
            send("col", put5.at[n, h], got5.at[n, h], SEND5 + 2 * n + h)
            got5[n, h, col] = put5[n, h, col]

    _, feed = growth_forcing_at_zero()
    for n, out in enumerate((s_out, a_out)):
        for h in range(2):
            whole("col", got5.at[n, h], SEND5 + 2 * n + h).wait_recv()
        weights = [back.at[k][...] for k in range(4)]
        blocks = [[got5[n, h, c] for c in range(COLS)] for h in range(2)]
        values = backward_columns(blocks, turn1[0], turn1[1], weights)
        for c in range(COLS):
            put6[n, c] = values[c] + feed if n == 0 else values[c]
        send("col", put6.at[n], out, SEND6 + n)
        out[col] = put6[n, col]

    for n, out in enumerate((s_out, a_out)):
        whole("col", out, SEND6 + n).wait_recv()
    for entry in pending:
        whole(*entry).wait_send()


def growth_forcing_at_zero():
    linear = -FEED_RATE
    return math.exp(HALF_STEP * linear), FEED_RATE * math.expm1(HALF_STEP * linear) / linear


def on_device(substrate, activator):
    wide, tall, turn1, turn2 = constants()
    shape = pltpu.VMEM((COLS, 8, WIDE), F32)
    held = lambda x: pltpu.with_memory_space_constraint(x, pltpu.HBM)
    anywhere = pl.BlockSpec(memory_space=pltpu.HBM)
    vmem = lambda *shape: pltpu.VMEM(shape, F32)
    by_col, by_tile = (COLS, 8, WIDE), (TILES, 8, LANES)
    half_col, half_row = (2, COLS, 8, LANES), (2, ROWS, 4, LANES)
    out = pl.pallas_call(
        kernel,
        name="section",
        out_shape=(shape, shape),
        in_specs=[anywhere] * 6,
        out_specs=(pl.BlockSpec(memory_space=pltpu.VMEM),) * 2,
        scratch_shapes=[
            vmem(2, *by_col),
            pltpu.VMEM(wide.shape, BF16),
            pltpu.VMEM(tall.shape, BF16),
            vmem(*turn1.shape),
            vmem(*turn2.shape),
            vmem(16, *by_tile),
            pltpu.VMEM(wide.shape, BF16),
            vmem(2, *by_col),
            vmem(3, *half_col),
            vmem(3, *half_col),
            vmem(3, *half_row),
            vmem(3, *half_row),
            vmem(*by_tile),
            vmem(3, 2, *by_tile),
            vmem(2 * TILES, 8, LANES),
            vmem(2 * TILES, 8, 2 * LANES),
            vmem(2, *half_row),
            vmem(2, *half_row),
            vmem(2, *half_col),
            vmem(2, *half_col),
            vmem(2, *by_col),
            pltpu.SemaphoreType.DMA((6,)),
            pltpu.SemaphoreType.DMA((24,)),
            pltpu.SemaphoreType.DMA((24,)),
        ],
        compiler_params=pltpu.CompilerParams(
            collective_id=0, has_side_effects=True, vmem_limit_bytes=20 << 20
        ),
    )(
        held(substrate.reshape(COLS, 8, WIDE)),
        held(activator.reshape(COLS, 8, WIDE)),
        held(jnp.asarray(wide)),
        held(jnp.asarray(tall)),
        held(jnp.asarray(turn1)),
        held(jnp.asarray(turn2)),
    )
    return tuple(x.reshape(substrate.shape) for x in out)


def solution(mesh):
    spec = P("row", "col")
    return jax.shard_map(
        on_device, mesh=mesh, in_specs=(spec, spec), out_specs=(spec, spec), check_vma=False
    )
```

```python
import math

import jax
import jax.numpy as jnp
import numpy as np
from jax import lax
from jax.experimental import pallas as pl
from jax.experimental.pallas import tpu as pltpu
from jax.sharding import PartitionSpec as P

FEED_RATE = 0.037
KILL_RATE = 0.06
HALF_STEP = 4.0
SUBSTRATE = (4e-07, FEED_RATE)
ACTIVATOR = (2e-07, FEED_RATE + KILL_RATE)
TOTAL = 4096
COLS = 16
ROWS = 32
WIDE = 256
LANES = 128
TILES = ROWS // 2
F32 = jnp.float32
BF16 = jnp.bfloat16


def c_add(a, b):
    im = a[1] if b[1] is None else (b[1] if a[1] is None else a[1] + b[1])
    return (a[0] + b[0], im)


def c_sub(a, b):
    im = a[1] if b[1] is None else (-b[1] if a[1] is None else a[1] - b[1])
    return (a[0] - b[0], im)


def c_conj(a):
    return (a[0], None if a[1] is None else -a[1])


def c_turn(a, numerator, denominator):
    numerator %= denominator
    if numerator == 0:
        return a
    if 4 * numerator == denominator:
        return (jnp.zeros_like(a[0]) if a[1] is None else -a[1], a[0])
    if 4 * numerator == 3 * denominator:
        return (jnp.zeros_like(a[0]) if a[1] is None else a[1], -a[0])
    cosine = math.cos(2.0 * math.pi * numerator / denominator)
    sine = math.sin(2.0 * math.pi * numerator / denominator)
    if a[1] is None:
        return (a[0] * cosine, a[0] * sine)
    return (a[0] * cosine - a[1] * sine, a[0] * sine + a[1] * cosine)


def real_forward(values):
    size = len(values)
    if size == 2:
        return [(values[0] + values[1], None), (values[0] - values[1], None)]
    even, odd = real_forward(values[::2]), real_forward(values[1::2])
    return join_halves(even, odd, size)


def join_halves(even, odd, size, first=0):
    half = size // 2
    out = [None] * (half + 1)
    for k in range(first, half // 2 + 1):
        turned = c_turn(odd[k], -k, size)
        out[k] = c_add(even[k], turned)
        if half - k != k:
            out[half - k] = c_conj(c_sub(even[k], turned))
    return out


def split_halves(spectrum, size, first=0):
    half = size // 2
    even, odd = [None] * (half // 2 + 1), [None] * (half // 2 + 1)
    for k in range(first, half // 2 + 1):
        if k == 0:
            even[k] = (spectrum[0][0] + spectrum[half][0], None)
            odd[k] = (spectrum[0][0] - spectrum[half][0], None)
        elif 2 * k == half:
            even[k] = (2.0 * spectrum[k][0], None)
            odd[k] = (-2.0 * spectrum[k][1], None)
        else:
            other = c_conj(spectrum[half - k])
            even[k] = c_add(spectrum[k], other)
            odd[k] = c_turn(c_sub(spectrum[k], other), k, size)
    return even, odd


def real_backward(spectrum):
    size = 2 * (len(spectrum) - 1)
    if size == 2:
        a, b = spectrum[0][0], spectrum[1][0]
        return [a + b, a - b]
    even, odd = split_halves(spectrum, size)
    even, odd = real_backward(even), real_backward(odd)
    return [x for pair in zip(even, odd) for x in pair]


def roll_rows(tile, shift):
    return pltpu.roll(tile, shift, 0)


def sublane():
    return lax.broadcasted_iota(jnp.int32, (8, LANES), 0)


def part_sign():
    return jnp.where(sublane() % 4 < 2, 1.0, -1.0).astype(F32)


def other_part(tile):
    return jnp.where(sublane() % 4 < 2, roll_rows(tile, 6), roll_rows(tile, 2))


def tile_turn(tile, cosine, signed_sine):
    return tile * cosine - signed_sine * other_part(tile)


def tile_fft(tiles, sign, direction):
    size = len(tiles)
    if size == 1:
        return tiles
    even, odd = tile_fft(tiles[::2], sign, direction), tile_fft(tiles[1::2], sign, direction)
    low, high = [], []
    for k in range(size // 2):
        turned = odd[k]
        if 4 * k == size:
            turned = (-direction * sign) * other_part(turned)
        elif k:
            angle = direction * 2.0 * math.pi * k / size
            turned = tile_turn(turned, math.cos(angle), sign * math.sin(angle))
        low.append(even[k] + turned)
        high.append(even[k] - turned)
    return low + high


def second_turn(tile, k, sign, direction):
    if k == 0:
        return tile
    angle = direction * 2.0 * math.pi * k / ROWS
    lower = sublane() < 4
    cosine = jnp.where(lower, 1.0, math.cos(angle)).astype(F32)
    sine = jnp.where(lower, 0.0, math.sin(angle)).astype(F32)
    return tile_turn(tile, cosine, sign * sine)


def block_sums(tile):
    return jnp.where(sublane() < 4, tile, -tile) + roll_rows(tile, 4)


def fft_down(tiles, sign):
    turned = [second_turn(x, k, sign, -1) for k, x in enumerate(tile_fft(tiles, sign, -1))]
    return [block_sums(x) for x in turned]


def fft_up(tiles, sign):
    turned = [second_turn(block_sums(x), k, sign, 1) for k, x in enumerate(tiles)]
    return tile_fft(turned, sign, 1)


MATRIX = (((1,), (0,)), ((), ()))


def pieces(values):
    top = values.astype(BF16)
    return top, (values - top.astype(F32)).astype(BF16)


def dot_wide(values, high, low):
    top, rest = pieces(values)
    size = values.shape[0]
    both = lax.dot_general(
        jnp.concatenate([top, rest], axis=0), high, MATRIX, preferred_element_type=F32
    )
    corner = lax.dot_general(top, low, MATRIX, preferred_element_type=F32)
    return both[:size] + (both[size:] + corner)


def dot_tall(values, matrix):
    top, rest = pieces(values)
    return lax.dot_general(
        jnp.concatenate([top, rest, top], axis=1), matrix, MATRIX, preferred_element_type=F32
    )


def forward_columns(values, turn_cos, turn_sin, weights):
    even, odd = real_forward(values[::2]), real_forward(values[1::2])
    spectrum = join_halves(even, odd, COLS, 1)
    rows = [jnp.concatenate([even[0][0], odd[0][0]], axis=1)]
    for k in range(1, COLS // 2):
        re, im = spectrum[k]
        cosine, sine = turn_cos[k : k + 1, :], turn_sin[k : k + 1, :]
        rows.append(jnp.concatenate([re * cosine + im * sine, im * cosine - re * sine], axis=1))
    stacked = jnp.concatenate(rows, axis=0)
    out = dot_wide(stacked, weights[0], weights[1])
    first = dot_wide(stacked[:16], weights[2], weights[3])
    blocks = [[], []]
    for slot in range(COLS // 2):
        row = first[:8] if slot == 0 else out[8 * slot : 8 * slot + 8]
        for n in range(4):
            blocks[n % 2].append(row[:, LANES * n : LANES * (n + 1)])
    return blocks


def backward_columns(blocks, turn_cos, turn_sin, weights):
    rows = []
    for s in range(COLS // 2):
        row = [blocks[0][2 * s], blocks[1][2 * s], blocks[0][2 * s + 1], blocks[1][2 * s + 1]]
        rows.append(jnp.concatenate(row, axis=1))
    stacked = jnp.concatenate(rows, axis=0)
    out = dot_wide(stacked, weights[0], weights[1])
    first = dot_wide(stacked[:16], weights[2], weights[3])
    spectrum = [None] * (COLS // 2)
    for k in range(1, COLS // 2):
        row = out[8 * k : 8 * k + 8]
        re, im = row[:, :WIDE], row[:, WIDE:]
        cosine, sine = turn_cos[k : k + 1, :], turn_sin[k : k + 1, :]
        spectrum[k] = (re * cosine - im * sine, im * cosine + re * sine)
    even, odd = split_halves(spectrum + [None], COLS, 1)
    even[0], odd[0] = (first[:8, :WIDE], None), (first[:8, WIDE:], None)
    even, odd = real_backward(even), real_backward(odd)
    return [x for pair in zip(even, odd) for x in pair]


def squared_wave(index):
    signed = jnp.where(2 * index < TOTAL, index, index - TOTAL).astype(F32)
    angular = (2.0 * math.pi) * signed
    return angular * angular


def growth_forcing(wave_number, diffusion, decay_rate):
    linear = -diffusion * wave_number - decay_rate
    growth = jnp.exp(HALF_STEP * linear)
    return growth, (growth - 1.0) / linear


def factors(step, half, row, col):
    column = 2 * half + sublane() % 2
    slot, side = col // 2, col % 2
    within = LANES * side + 4 * row + column
    q = jnp.where(slot == 0, 8 * within, slot + COLS * within)
    p = step + TILES * (sublane() // 4) + ROWS * lax.broadcasted_iota(jnp.int32, (8, LANES), 1)
    row_wave = squared_wave(p)
    wave_number = row_wave + squared_wave(q)
    last = row_wave + (2.0 * math.pi * (TOTAL // 2)) ** 2
    norm = 1.0 / (TOTAL * TOTAL)
    paired = jnp.where(q == 0, 1.0, jnp.where(slot == 0, 2.0, 1.0)).astype(F32)
    out = []
    for species, sign in ((SUBSTRATE, -1.0), (ACTIVATOR, 1.0)):
        for waves, scale in ((wave_number, paired * norm), (last, norm))[: 2 - half]:
            growth, forcing = growth_forcing(waves, *species)
            out += [growth * scale, forcing * (scale * sign)]
    return out


def constants():
    def split(matrix):
        high = matrix.astype(np.float32).astype(BF16)
        return high, (matrix - high.astype(np.float64)).astype(np.float32).astype(BF16)

    def interleave(re, im):
        both = np.stack([re, im], axis=1).reshape(-1, 2, 2, ROWS, 2, 2)
        return both.transpose(0, 2, 4, 3, 1, 5).reshape(re.shape[0], -1)

    j = np.arange(WIDE)
    angle = 2.0 * np.pi * (np.outer(j, j) % WIDE) / WIDE
    cos, sin = np.cos(angle), np.sin(angle)
    pair = interleave(np.concatenate([cos, sin]), np.concatenate([-sin, cos]))
    long = np.arange(2 * WIDE)
    angle = 2.0 * np.pi * (np.outer(long, j) % (2 * WIDE)) / (2 * WIDE)
    cos, sin = np.cos(angle), -np.sin(angle)
    sin[:, 0] = 1.0 - 2.0 * (long % 2)
    single = interleave(cos, sin)
    wide = np.stack([*split(pair), *split(single)])
    i = np.arange(LANES)
    angle = 2.0 * np.pi * (np.outer(i, i) % LANES) / LANES
    high, low = split(np.concatenate([np.cos(angle), np.sin(angle)], axis=1))
    tall = np.concatenate([high, high, low])

    angle = 2.0 * np.pi * np.outer(np.arange(COLS // 2), j) / TOTAL
    turn1 = np.stack([np.cos(angle), np.sin(angle)]).astype(np.float32)
    block, part, _ = np.unravel_index(np.arange(8), (2, 2, 2))
    wave = np.arange(TILES)[:, None] + TILES * block
    angle = 2.0 * np.pi * wave[:, :, None] * i / TOTAL
    sign = np.where(part == 0, 1.0, -1.0)[:, None]
    turn2 = np.stack([np.cos(angle), sign * np.sin(angle)]).astype(np.float32)
    return wide, tall, turn1, turn2


SEND1, SEND2, SEND3, SEND4, SEND5, SEND6 = 0, 2, 8, 14, 18, 22
U, R, V = 0, 1, 2


def kernel(
    u_hbm, v_hbm, wide_hbm, tall_hbm, turn1_hbm, turn2_hbm, s_out, a_out,
    fields, wide, tall, turn1, turn2, tables, back,
    got1, put2, got2, put3, got3, tiles, spectra, pair, products,
    put4, got4, put5, got5, put6, local_sem, send_sem, recv_sem,
):
    row, col = lax.axis_index("row"), lax.axis_index("col")
    mesh_id = pl.DeviceIdType.MESH

    loads = [
        pltpu.make_async_copy(src, dst, local_sem.at[n])
        for n, (src, dst) in enumerate(
            [
                (u_hbm, fields.at[0]),
                (v_hbm, fields.at[1]),
                (wide_hbm, wide),
                (tall_hbm, tall),
                (turn1_hbm, turn1),
                (turn2_hbm, turn2),
            ]
        )
    ]
    for load in loads:
        load.start()

    barrier = pltpu.get_barrier_semaphore()

    def greet(axis, me, size):
        def body(peer, carry):
            pl.semaphore_signal(barrier, inc=1, device_id={axis: peer}, device_id_type=mesh_id)
            return carry

        lax.fori_loop(me + 1, size, body, 0)
        lax.fori_loop(0, me, body, 0)

    pending = []

    def piece(axis, peer, source, target, sem):
        return pltpu.make_async_remote_copy(
            src_ref=source,
            dst_ref=target,
            send_sem=send_sem.at[sem],
            recv_sem=recv_sem.at[sem],
            device_id={axis: peer},
            device_id_type=mesh_id,
        )

    def send(axis, source, target, sem):
        me, size = (col, COLS) if axis == "col" else (row, ROWS)

        def body(peer, carry):
            piece(axis, peer, source.at[peer], target.at[me], sem).start()
            return carry

        lax.fori_loop(me + 1, size, body, 0)
        lax.fori_loop(0, me, body, 0)
        pending.append((axis, source, sem))

    def whole(axis, block, sem):
        me, size = (col, COLS) if axis == "col" else (row, ROWS)
        block = block.at[pl.ds(0, size - 1)]
        return piece(axis, lax.rem(me + 1, size), block, block, sem)

    greet("col", col, COLS)
    greet("row", row, ROWS)
    loads[0].wait()
    pl.semaphore_wait(barrier, COLS - 1 + ROWS - 1)

    for n in range(2):
        if n == 1:
            loads[1].wait()
        send("col", fields.at[n], got1.at[n], SEND1 + n)
        got1[n, col] = fields[n, col]

    def fill(step, carry):
        for half in range(2):
            for n, table in enumerate(factors(step, half, row, col)):
                tables[8 * half + n, step] = table
        return carry

    lax.fori_loop(0, TILES, fill, 0)

    def forward_rows(n, values):
        blocks = forward_columns(
            values, turn1[0], turn1[1], [wide.at[k][...] for k in range(4)]
        )
        for h in range(2):
            for c in range(COLS):
                put2[n, h, c] = blocks[h][c]
            send("col", put2.at[n, h], got2.at[n, h], SEND2 + 2 * n + h)
            got2[n, h, col] = put2[n, h, col]

    for load in loads[2:]:
        load.wait()
    whole("col", got1.at[0], SEND1).wait_recv()
    forward_rows(U, [got1[0, c] for c in range(COLS)])
    whole("col", got1.at[1], SEND1 + 1).wait_recv()
    forward_rows(R, [got1[0, c] * got1[1, c] * got1[1, c] for c in range(COLS)])
    forward_rows(V, [got1[1, c] for c in range(COLS)])

    for n in (U, R, V):
        for h in range(2):
            whole("col", got2.at[n, h], SEND2 + 2 * n + h).wait_recv()
            turned = got2[n, h].reshape(LANES, LANES).T
            for r in range(ROWS):
                put3[n, h, r] = turned[4 * r : 4 * r + 4]
            send("row", put3.at[n, h], got3.at[n, h], SEND3 + 2 * n + h)
            got3[n, h, row] = put3[n, h, row]

    sign = part_sign()

    def two_blocks(ref, t):
        return jnp.concatenate([ref[2 * t], ref[2 * t + 1]], axis=0)

    def forward_down(n, h):
        whole("row", got3.at[n, h], SEND3 + 2 * n + h).wait_recv()
        values = fft_down([two_blocks(got3.at[n, h], t) for t in range(TILES)], sign)
        for k in range(TILES):
            tiles[k] = tile_turn(values[k], turn2[0, k], -turn2[1, k])
        out = dot_tall(tiles[...].reshape(LANES, LANES), tall[...])
        products[pl.ds(0, TILES)] = out.reshape(TILES, 8, 2 * LANES)
        for k in range(TILES):
            both = products[k]
            spectra[n, h, k] = both[:, :LANES] + sign * other_part(both[:, LANES:])

    special = sublane() % 4 == jnp.where(row + col == 0, 2, -1)

    def backward_down(n, field, h):
        parts = 2 - h
        for k in range(TILES):
            own, source = spectra[field, h, k], spectra[R, h, k]
            for m in range(parts):
                t = 8 * h + 2 * (parts * n + m)
                pair[m * TILES + k] = tables[t, k] * own + tables[t + 1, k] * source
        block = pair[pl.ds(0, parts * TILES)].reshape(parts * LANES, LANES)
        out = dot_tall(block, tall[...])
        products[pl.ds(0, parts * TILES)] = out.reshape(parts * TILES, 8, 2 * LANES)
        for m in reversed(range(parts)):
            turned = []
            for k in range(TILES):
                both = products[m * TILES + k]
                tile = both[:, :LANES] - sign * other_part(both[:, LANES:])
                turned.append(tile_turn(tile, turn2[0, k], turn2[1, k]))
            values = fft_up(turned, sign)
            for t in range(TILES):
                value = values[t]
                if m == 1:
                    tiles[t] = value
                    continue
                if h == 0:
                    value = jnp.where(special, tiles[t], value)
                put4[n, h, 2 * t] = value[:4]
                put4[n, h, 2 * t + 1] = value[4:]
        send("row", put4.at[n, h], got4.at[n, h], SEND4 + 2 * n + h)
        got4[n, h, row] = put4[n, h, row]

    forward_down(U, 0)
    forward_down(U, 1)
    for h in range(2):
        forward_down(R, h)
        backward_down(0, U, h)
    for h in range(2):
        forward_down(V, h)
        backward_down(1, V, h)

    for k in range(4):
        back[k] = wide.at[k][...].T

    for n in range(2):
        for h in range(2):
            whole("row", got4.at[n, h], SEND4 + 2 * n + h).wait_recv()
            block = jnp.concatenate([two_blocks(got4.at[n, h], t) for t in range(TILES)], axis=0)
            put5[n, h] = block.T.reshape(COLS, 8, LANES)
            send("col", put5.at[n, h], got5.at[n, h], SEND5 + 2 * n + h)
            got5[n, h, col] = put5[n, h, col]

    _, feed = growth_forcing_at_zero()
    for n, out in enumerate((s_out, a_out)):
        for h in range(2):
            whole("col", got5.at[n, h], SEND5 + 2 * n + h).wait_recv()
        weights = [back.at[k][...] for k in range(4)]
        blocks = [[got5[n, h, c] for c in range(COLS)] for h in range(2)]
        values = backward_columns(blocks, turn1[0], turn1[1], weights)
        for c in range(COLS):
            put6[n, c] = values[c] + feed if n == 0 else values[c]
        send("col", put6.at[n], out, SEND6 + n)
        out[col] = put6[n, col]

    for n, out in enumerate((s_out, a_out)):
        whole("col", out, SEND6 + n).wait_recv()
    for entry in pending:
        whole(*entry).wait_send()


def store_kernel(s_ref, a_ref, s_out, a_out, sems):
    copies = [
        pltpu.make_async_copy(s_ref, s_out, sems.at[0]),
        pltpu.make_async_copy(a_ref, a_out, sems.at[1]),
    ]
    for copy in copies:
        copy.start()
    for copy in copies:
        copy.wait()


def growth_forcing_at_zero():
    linear = -FEED_RATE
    return math.exp(HALF_STEP * linear), FEED_RATE * math.expm1(HALF_STEP * linear) / linear


def on_device(substrate, activator):
    wide, tall, turn1, turn2 = constants()
    shape = pltpu.VMEM((COLS, 8, WIDE), F32)
    held = lambda x: pltpu.with_memory_space_constraint(x, pltpu.HBM)
    anywhere = pl.BlockSpec(memory_space=pltpu.HBM)
    vmem = lambda *shape: pltpu.VMEM(shape, F32)
    by_col, by_tile = (COLS, 8, WIDE), (TILES, 8, LANES)
    half_col, half_row = (2, COLS, 8, LANES), (2, ROWS, 4, LANES)
    out = pl.pallas_call(
        kernel,
        name="section",
        out_shape=(shape, shape),
        in_specs=[anywhere] * 6,
        out_specs=(pl.BlockSpec(memory_space=pltpu.VMEM),) * 2,
        scratch_shapes=[
            vmem(2, *by_col),
            pltpu.VMEM(wide.shape, BF16),
            pltpu.VMEM(tall.shape, BF16),
            vmem(*turn1.shape),
            vmem(*turn2.shape),
            vmem(16, *by_tile),
            pltpu.VMEM(wide.shape, BF16),
            vmem(2, *by_col),
            vmem(3, *half_col),
            vmem(3, *half_col),
            vmem(3, *half_row),
            vmem(3, *half_row),
            vmem(*by_tile),
            vmem(3, 2, *by_tile),
            vmem(2 * TILES, 8, LANES),
            vmem(2 * TILES, 8, 2 * LANES),
            vmem(2, *half_row),
            vmem(2, *half_row),
            vmem(2, *half_col),
            vmem(2, *half_col),
            vmem(2, *by_col),
            pltpu.SemaphoreType.DMA((6,)),
            pltpu.SemaphoreType.DMA((24,)),
            pltpu.SemaphoreType.DMA((24,)),
        ],
        compiler_params=pltpu.CompilerParams(
            collective_id=0, has_side_effects=True, vmem_limit_bytes=20 << 20
        ),
    )(
        held(substrate.reshape(COLS, 8, WIDE)),
        held(activator.reshape(COLS, 8, WIDE)),
        held(jnp.asarray(wide)),
        held(jnp.asarray(tall)),
        held(jnp.asarray(turn1)),
        held(jnp.asarray(turn2)),
    )
    flat = jax.ShapeDtypeStruct(substrate.shape, F32)
    return pl.pallas_call(
        store_kernel,
        name="store",
        out_shape=(flat, flat),
        in_specs=[pl.BlockSpec(memory_space=pltpu.VMEM)] * 2,
        out_specs=(pl.BlockSpec(memory_space=pltpu.HBM),) * 2,
        scratch_shapes=[pltpu.SemaphoreType.DMA((2,))],
    )(*(pltpu.with_memory_space_constraint(x.reshape(substrate.shape), pltpu.VMEM) for x in out))


def solution(mesh):
    spec = P("row", "col")
    return jax.shard_map(
        on_device, mesh=mesh, in_specs=(spec, spec), out_specs=(spec, spec), check_vma=False
    )
```

```python
import math

import jax
import jax.numpy as jnp
import numpy as np
from jax import lax
from jax.experimental import pallas as pl
from jax.experimental.pallas import tpu as pltpu
from jax.sharding import PartitionSpec as P

FEED_RATE = 0.037
KILL_RATE = 0.06
HALF_STEP = 4.0
SUBSTRATE = (4e-07, FEED_RATE)
ACTIVATOR = (2e-07, FEED_RATE + KILL_RATE)
TOTAL = 4096
COLS = 16
ROWS = 32
WIDE = 256
LANES = 128
TILES = ROWS // 2
F32 = jnp.float32
BF16 = jnp.bfloat16


def c_add(a, b):
    im = a[1] if b[1] is None else (b[1] if a[1] is None else a[1] + b[1])
    return (a[0] + b[0], im)


def c_sub(a, b):
    im = a[1] if b[1] is None else (-b[1] if a[1] is None else a[1] - b[1])
    return (a[0] - b[0], im)


def c_conj(a):
    return (a[0], None if a[1] is None else -a[1])


def c_turn(a, numerator, denominator):
    numerator %= denominator
    if numerator == 0:
        return a
    if 4 * numerator == denominator:
        return (jnp.zeros_like(a[0]) if a[1] is None else -a[1], a[0])
    if 4 * numerator == 3 * denominator:
        return (jnp.zeros_like(a[0]) if a[1] is None else a[1], -a[0])
    cosine = math.cos(2.0 * math.pi * numerator / denominator)
    sine = math.sin(2.0 * math.pi * numerator / denominator)
    if a[1] is None:
        return (a[0] * cosine, a[0] * sine)
    return (a[0] * cosine - a[1] * sine, a[0] * sine + a[1] * cosine)


def real_forward(values):
    size = len(values)
    if size == 2:
        return [(values[0] + values[1], None), (values[0] - values[1], None)]
    even, odd = real_forward(values[::2]), real_forward(values[1::2])
    return join_halves(even, odd, size)


def join_halves(even, odd, size, first=0):
    half = size // 2
    out = [None] * (half + 1)
    for k in range(first, half // 2 + 1):
        turned = c_turn(odd[k], -k, size)
        out[k] = c_add(even[k], turned)
        if half - k != k:
            out[half - k] = c_conj(c_sub(even[k], turned))
    return out


def split_halves(spectrum, size, first=0):
    half = size // 2
    even, odd = [None] * (half // 2 + 1), [None] * (half // 2 + 1)
    for k in range(first, half // 2 + 1):
        if k == 0:
            even[k] = (spectrum[0][0] + spectrum[half][0], None)
            odd[k] = (spectrum[0][0] - spectrum[half][0], None)
        elif 2 * k == half:
            even[k] = (2.0 * spectrum[k][0], None)
            odd[k] = (-2.0 * spectrum[k][1], None)
        else:
            other = c_conj(spectrum[half - k])
            even[k] = c_add(spectrum[k], other)
            odd[k] = c_turn(c_sub(spectrum[k], other), k, size)
    return even, odd


def real_backward(spectrum):
    size = 2 * (len(spectrum) - 1)
    if size == 2:
        a, b = spectrum[0][0], spectrum[1][0]
        return [a + b, a - b]
    even, odd = split_halves(spectrum, size)
    even, odd = real_backward(even), real_backward(odd)
    return [x for pair in zip(even, odd) for x in pair]


def roll_rows(tile, shift):
    return pltpu.roll(tile, shift, 0)


def sublane():
    return lax.broadcasted_iota(jnp.int32, (8, LANES), 0)


def part_sign():
    return jnp.where(sublane() % 4 < 2, 1.0, -1.0).astype(F32)


def other_part(tile):
    return jnp.where(sublane() % 4 < 2, roll_rows(tile, 6), roll_rows(tile, 2))


def tile_turn(tile, cosine, signed_sine):
    return tile * cosine - signed_sine * other_part(tile)


def tile_fft(tiles, sign, direction):
    size = len(tiles)
    if size == 1:
        return tiles
    even, odd = tile_fft(tiles[::2], sign, direction), tile_fft(tiles[1::2], sign, direction)
    low, high = [], []
    for k in range(size // 2):
        turned = odd[k]
        if 4 * k == size:
            turned = (-direction * sign) * other_part(turned)
        elif k:
            angle = direction * 2.0 * math.pi * k / size
            turned = tile_turn(turned, math.cos(angle), sign * math.sin(angle))
        low.append(even[k] + turned)
        high.append(even[k] - turned)
    return low + high


def second_turn(tile, k, sign, direction):
    if k == 0:
        return tile
    angle = direction * 2.0 * math.pi * k / ROWS
    lower = sublane() < 4
    cosine = jnp.where(lower, 1.0, math.cos(angle)).astype(F32)
    sine = jnp.where(lower, 0.0, math.sin(angle)).astype(F32)
    return tile_turn(tile, cosine, sign * sine)


def block_sums(tile):
    return jnp.where(sublane() < 4, tile, -tile) + roll_rows(tile, 4)


def fft_down(tiles, sign):
    turned = [second_turn(x, k, sign, -1) for k, x in enumerate(tile_fft(tiles, sign, -1))]
    return [block_sums(x) for x in turned]


def fft_up(tiles, sign):
    turned = [second_turn(block_sums(x), k, sign, 1) for k, x in enumerate(tiles)]
    return tile_fft(turned, sign, 1)


MATRIX = (((1,), (0,)), ((), ()))


def pieces(values):
    top = values.astype(BF16)
    return top, (values - top.astype(F32)).astype(BF16)


def dot_wide(values, high, low):
    top, rest = pieces(values)
    size = values.shape[0]
    both = lax.dot_general(
        jnp.concatenate([top, rest], axis=0), high, MATRIX, preferred_element_type=F32
    )
    corner = lax.dot_general(top, low, MATRIX, preferred_element_type=F32)
    return both[:size] + (both[size:] + corner)


def dot_tall(values, matrix):
    top, rest = pieces(values)
    return lax.dot_general(
        jnp.concatenate([top, rest, top], axis=1), matrix, MATRIX, preferred_element_type=F32
    )


def forward_columns(values, turn_cos, turn_sin, weights):
    even, odd = real_forward(values[::2]), real_forward(values[1::2])
    spectrum = join_halves(even, odd, COLS, 1)
    rows = [jnp.concatenate([even[0][0], odd[0][0]], axis=1)]
    for k in range(1, COLS // 2):
        re, im = spectrum[k]
        cosine, sine = turn_cos[k : k + 1, :], turn_sin[k : k + 1, :]
        rows.append(jnp.concatenate([re * cosine + im * sine, im * cosine - re * sine], axis=1))
    stacked = jnp.concatenate(rows, axis=0)
    out = dot_wide(stacked, weights[0], weights[1])
    first = dot_wide(stacked[:16], weights[2], weights[3])
    return [first[:8]] + [out[8 * slot : 8 * slot + 8] for slot in range(1, COLS // 2)]


def backward_columns(blocks, added, turn_cos, turn_sin, weights):
    rows = []
    for s in range(COLS // 2):
        row = [blocks[0][2 * s], blocks[1][2 * s], blocks[0][2 * s + 1], blocks[1][2 * s + 1]]
        rows.append(jnp.concatenate(row, axis=1) + added[s])
    stacked = jnp.concatenate(rows, axis=0)
    out = dot_wide(stacked, weights[0], weights[1])
    first = dot_wide(stacked[:16], weights[2], weights[3])
    spectrum = [None] * (COLS // 2)
    for k in range(1, COLS // 2):
        row = out[8 * k : 8 * k + 8]
        re, im = row[:, :WIDE], row[:, WIDE:]
        cosine, sine = turn_cos[k : k + 1, :], turn_sin[k : k + 1, :]
        spectrum[k] = (re * cosine - im * sine, im * cosine + re * sine)
    even, odd = split_halves(spectrum + [None], COLS, 1)
    even[0], odd[0] = (first[:8, :WIDE], None), (first[:8, WIDE:], None)
    even, odd = real_backward(even), real_backward(odd)
    return [x for pair in zip(even, odd) for x in pair]


def squared_wave(index):
    signed = jnp.where(2 * index < TOTAL, index, index - TOTAL).astype(F32)
    angular = (2.0 * math.pi) * signed
    return angular * angular


def forcing_of(wave_number, diffusion, decay_rate):
    linear = -diffusion * wave_number - decay_rate
    return (jnp.exp(HALF_STEP * linear) - 1.0) / linear


def forcings(step, half, row, col):
    column = sublane() % 2
    slot, side = col // 2, col % 2
    within = LANES * side + 4 * row + 2 * half + column
    q = jnp.where(slot == 0, 8 * within, slot + COLS * within)
    p = step + TILES * (sublane() // 4) + ROWS * lax.broadcasted_iota(jnp.int32, (8, LANES), 1)
    row_wave = squared_wave(p)
    wave_number = row_wave + squared_wave(q)
    norm = 1.0 / (TOTAL * TOTAL)
    scale = jnp.where(q == 0, norm, jnp.where(slot == 0, 2.0 * norm, norm)).astype(F32)
    out = [
        -scale * forcing_of(wave_number, *SUBSTRATE),
        scale * forcing_of(wave_number, *ACTIVATOR),
    ]
    if half == 0:
        last = row_wave + (2.0 * math.pi * (TOTAL // 2)) ** 2
        first = -norm * forcing_of(last, *SUBSTRATE)
        out.append(jnp.where(column == 0, first, norm * forcing_of(last, *ACTIVATOR)))
    return out


def column_growth(index, diffusion):
    angular = 2.0 * np.pi * np.where(2 * index < TOTAL, index, index - TOTAL)
    return np.exp(-HALF_STEP * diffusion * angular * angular)


def constants():
    def split(matrix):
        high = matrix.astype(np.float32).astype(BF16)
        return high, (matrix - high.astype(np.float64)).astype(np.float32).astype(BF16)

    def interleave(re, im):
        both = np.stack([re, im], axis=1).reshape(-1, 2, 2, ROWS, 2, 2)
        return both.transpose(0, 2, 4, 3, 1, 5).reshape(re.shape[0], -1)

    j = np.arange(WIDE)
    angle = 2.0 * np.pi * (np.outer(j, j) % WIDE) / WIDE
    cos, sin = np.cos(angle), np.sin(angle)
    pair = interleave(np.concatenate([cos, sin]), np.concatenate([-sin, cos]))
    long = np.arange(2 * WIDE)
    angle = 2.0 * np.pi * (np.outer(long, j) % (2 * WIDE)) / (2 * WIDE)
    cos, sin = np.cos(angle), -np.sin(angle)
    sin[:, 0] = 1.0 - 2.0 * (long % 2)
    single = interleave(cos, sin)
    wide = np.stack([*split(pair), *split(single)])
    i = np.arange(LANES)
    angle = 2.0 * np.pi * (np.outer(i, i) % LANES) / LANES
    high, low = split(np.concatenate([np.cos(angle), np.sin(angle)], axis=1))
    tall = np.concatenate([high, high, low])

    angle = 2.0 * np.pi * np.outer(np.arange(COLS // 2), j) / TOTAL
    turn1 = np.stack([np.cos(angle), np.sin(angle)]).astype(np.float32)
    block, part, _ = np.unravel_index(np.arange(8), (2, 2, 2))
    wave = np.arange(TILES)[:, None] + TILES * block
    angle = 2.0 * np.pi * wave[:, :, None] * i / TOTAL
    sign = np.where(part == 0, 1.0, -1.0)[:, None]
    turn2 = np.stack([np.cos(angle), sign * np.sin(angle)]).astype(np.float32)
    rows = np.arange(ROWS)[:, None] + ROWS * i
    angle = 2.0 * np.pi * np.arange(ROWS)[:, None] * i / TOTAL
    down = [np.cos(angle), np.sin(angle)]
    slot = np.arange(COLS // 2)[:, None]
    q = np.where(slot == 0, 8 * j, slot + COLS * j)
    last = np.where(q == 0, TOTAL // 2, q)
    paired = np.where(slot == 0, 2.0, 1.0)
    across = []
    for diffusion, decay_rate in (SUBSTRATE, ACTIVATOR):
        down.append(column_growth(rows, diffusion) / TOTAL)
        decay = math.exp(-HALF_STEP * decay_rate) / TOTAL
        parts = [
            np.where(q == 0, 1.0, paired) * column_growth(waves, diffusion) * decay
            for waves in (q, last)
        ]
        across.append(interleave(*parts))
    down, across = np.stack(down).astype(np.float32), np.stack(across).astype(np.float32)
    return wide, tall, turn1, turn2, down, across


SEND1, SEND2, SEND3, SEND4, SEND5, SEND6 = 0, 1, 3, 5, 9, 13
SENDA, SENDB, SENDC = 15, 17, 19


def kernel(
    u_hbm, v_hbm, wide_hbm, tall_hbm, turn1_hbm, turn2_hbm, down_hbm, across_hbm, s_out, a_out,
    fields, wide, tall, turn1, turn2, down, across, tables, back,
    got1, put2, got2, put3, got3, tiles, spectra, pair, products, extra,
    put4, got4, put5, got5, put6,
    put_a, got_a, put_b, got_b, put_c, got_c, grown, local_sem, send_sem, recv_sem,
):
    row, col = lax.axis_index("row"), lax.axis_index("col")
    mesh_id = pl.DeviceIdType.MESH

    loads = [
        pltpu.make_async_copy(src, dst, local_sem.at[n])
        for n, (src, dst) in enumerate(
            [
                (u_hbm, fields.at[0]),
                (v_hbm, fields.at[1]),
                (wide_hbm, wide),
                (tall_hbm, tall),
                (turn1_hbm, turn1),
                (turn2_hbm, turn2),
                (down_hbm, down),
                (across_hbm, across),
            ]
        )
    ]
    for load in loads:
        load.start()

    barrier = pltpu.get_barrier_semaphore()

    def greet(axis, me, size):
        def body(peer, carry):
            pl.semaphore_signal(barrier, inc=1, device_id={axis: peer}, device_id_type=mesh_id)
            return carry

        lax.fori_loop(me + 1, size, body, 0)
        lax.fori_loop(0, me, body, 0)

    pending = []

    def piece(axis, peer, source, target, sem):
        return pltpu.make_async_remote_copy(
            src_ref=source,
            dst_ref=target,
            send_sem=send_sem.at[sem],
            recv_sem=recv_sem.at[sem],
            device_id={axis: peer},
            device_id_type=mesh_id,
        )

    def send(axis, source, target, sem):
        me, size = (col, COLS) if axis == "col" else (row, ROWS)

        def body(peer, carry):
            piece(axis, peer, source.at[peer], target.at[me], sem).start()
            return carry

        lax.fori_loop(me + 1, size, body, 0)
        lax.fori_loop(0, me, body, 0)
        pending.append((axis, source, sem))

    def whole(axis, block, sem):
        me, size = (col, COLS) if axis == "col" else (row, ROWS)
        block = block.at[pl.ds(0, size - 1)]
        return piece(axis, lax.rem(me + 1, size), block, block, sem)

    greet("col", col, COLS)
    greet("row", row, ROWS)
    loads[0].wait()
    loads[1].wait()
    fields[2] = fields[0] * fields[1] * fields[1]
    pl.semaphore_wait(barrier, COLS - 1 + ROWS - 1)

    sign = part_sign()

    send("col", fields.at[2], got1, SEND1)
    got1[col] = fields[2, col]

    for n in range(2):
        put_a[n] = fields[n].reshape(LANES, WIDE).T.reshape(ROWS, 8, LANES)
        send("row", put_a.at[n], got_a.at[n], SENDA + n)
        got_a[n, row] = put_a[n, row]

    def fill(step, carry):
        for half in range(2):
            for n, table in enumerate(forcings(step, half, row, col)):
                tables[3 * half + n, step] = table
        return carry

    lax.fori_loop(0, TILES, fill, 0)
    for load in loads[2:]:
        load.wait()

    def spectrum_of(values):
        weights = [wide.at[k][...] for k in range(4)]
        return forward_columns(values, turn1[0], turn1[1], weights)

    whole("col", got1, SEND1).wait_recv()
    rows = spectrum_of([got1[c] for c in range(COLS)])
    for h in range(2):
        for c in range(COLS):
            start = WIDE * (c % 2) + LANES * h
            put2[h, c] = rows[c // 2][:, start : start + LANES]
        send("col", put2.at[h], got2.at[h], SEND2 + h)
        got2[h, col] = put2[h, col]

    def filter_columns(n):
        whole("row", got_a.at[n], SENDA + n).wait_recv()
        values = tile_fft([got_a[n, r] for r in range(ROWS)], sign, -1)
        for k in range(ROWS):
            cosine, sine = down[0, k : k + 1, :], sign * down[1, k : k + 1, :]
            pair[k] = tile_turn(values[k], cosine, -sine)
        out = dot_tall(pair[...].reshape(ROWS * 8, LANES), tall[...])
        products[pl.ds(0, ROWS)] = out.reshape(ROWS, 8, 2 * LANES)
        for k in range(ROWS):
            both = products[k]
            wave = both[:, :LANES] + sign * other_part(both[:, LANES:])
            pair[k] = wave * down[2 + n, k : k + 1, :]
        out = dot_tall(pair[...].reshape(ROWS * 8, LANES), tall[...])
        products[pl.ds(0, ROWS)] = out.reshape(ROWS, 8, 2 * LANES)
        turned = []
        for k in range(ROWS):
            both = products[k]
            tile = both[:, :LANES] - sign * other_part(both[:, LANES:])
            cosine, sine = down[0, k : k + 1, :], sign * down[1, k : k + 1, :]
            turned.append(tile_turn(tile, cosine, sine))
        values = tile_fft(turned, sign, 1)
        for r in range(ROWS):
            put_b[n, r] = values[r]
        send("row", put_b.at[n], got_b.at[n], SENDB + n)
        got_b[n, row] = put_b[n, row]

    def send_rows(n):
        whole("row", got_b.at[n], SENDB + n).wait_recv()
        put_c[n] = got_b[n].reshape(WIDE, LANES).T.reshape(COLS, 8, WIDE)
        send("col", put_c.at[n], got_c.at[n], SENDC + n)
        got_c[n, col] = put_c[n, col]

    def grow(n):
        whole("col", got_c.at[n], SENDC + n).wait_recv()
        rows = spectrum_of([got_c[n, c] for c in range(COLS)])
        for s in range(COLS // 2):
            grown[n, s] = rows[s] * across[n, s : s + 1, :]

    def turn_columns(h):
        whole("col", got2.at[h], SEND2 + h).wait_recv()
        turned = got2[h].reshape(LANES, LANES).T
        for r in range(ROWS):
            put3[h, r] = turned[4 * r : 4 * r + 4]
        send("row", put3.at[h], got3.at[h], SEND3 + h)
        got3[h, row] = put3[h, row]

    def two_blocks(ref, t):
        return jnp.concatenate([ref[2 * t], ref[2 * t + 1]], axis=0)

    def forward_down(h):
        whole("row", got3.at[h], SEND3 + h).wait_recv()
        values = fft_down([two_blocks(got3.at[h], t) for t in range(TILES)], sign)
        for k in range(TILES):
            tiles[k] = tile_turn(values[k], turn2[0, k], -turn2[1, k])
        out = dot_tall(tiles[...].reshape(LANES, LANES), tall[...])
        products[pl.ds(0, TILES)] = out.reshape(TILES, 8, 2 * LANES)
        for k in range(TILES):
            both = products[k]
            spectra[h, k] = both[:, :LANES] + sign * other_part(both[:, LANES:])

    special = sublane() % 4 == jnp.where(row + col == 0, 2, -1)

    def backward_down(n, h):
        parts = 2 if n == 0 and h == 0 else 1
        for k in range(TILES):
            wave = spectra[h, k]
            pair[k] = tables[3 * h + n, k] * wave
            if parts == 2:
                both = jnp.where(sublane() % 2 == 0, wave, roll_rows(wave, 1))
                pair[TILES + k] = tables[2, k] * both
        block = pair[pl.ds(0, parts * TILES)].reshape(parts * LANES, LANES)
        out = dot_tall(block, tall[...])
        products[pl.ds(0, parts * TILES)] = out.reshape(parts * TILES, 8, 2 * LANES)
        for m in reversed(range(parts)):
            turned = []
            for k in range(TILES):
                both = products[m * TILES + k]
                tile = both[:, :LANES] - sign * other_part(both[:, LANES:])
                turned.append(tile_turn(tile, turn2[0, k], turn2[1, k]))
            values = fft_up(turned, sign)
            for t in range(TILES):
                value = values[t]
                if m == 1:
                    extra[t] = value
                    continue
                if h == 0:
                    fixed = extra[t] if n == 0 else roll_rows(extra[t], 7)
                    value = jnp.where(special, fixed, value)
                put4[n, h, 2 * t] = value[:4]
                put4[n, h, 2 * t + 1] = value[4:]
        send("row", put4.at[n, h], got4.at[n, h], SEND4 + 2 * n + h)
        got4[n, h, row] = put4[n, h, row]

    def turn_back(n, h):
        whole("row", got4.at[n, h], SEND4 + 2 * n + h).wait_recv()
        block = jnp.concatenate([two_blocks(got4.at[n, h], t) for t in range(TILES)], axis=0)
        put5[n, h] = block.T.reshape(COLS, 8, LANES)
        send("col", put5.at[n, h], got5.at[n, h], SEND5 + 2 * n + h)
        got5[n, h, col] = put5[n, h, col]

    filter_columns(0)
    filter_columns(1)
    for k in range(4):
        back[k] = wide.at[k][...].T
    turn_columns(0)
    turn_columns(1)
    send_rows(0)
    forward_down(0)
    backward_down(0, 0)
    forward_down(1)
    backward_down(0, 1)
    send_rows(1)
    backward_down(1, 0)
    backward_down(1, 1)
    grow(0)
    for n in range(2):
        for h in range(2):
            turn_back(n, h)
    grow(1)

    feed = feed_forcing()
    for n, out in enumerate((s_out, a_out)):
        for h in range(2):
            whole("col", got5.at[n, h], SEND5 + 2 * n + h).wait_recv()
        weights = [back.at[k][...] for k in range(4)]
        blocks = [[got5[n, h, c] for c in range(COLS)] for h in range(2)]
        added = [grown[n, s] for s in range(COLS // 2)]
        values = backward_columns(blocks, added, turn1[0], turn1[1], weights)
        for c in range(COLS):
            put6[n, c] = values[c] + feed if n == 0 else values[c]
        send("col", put6.at[n], out, SEND6 + n)
        out[col] = put6[n, col]

    for n, out in enumerate((s_out, a_out)):
        whole("col", out, SEND6 + n).wait_recv()
    for entry in pending:
        whole(*entry).wait_send()


def store_kernel(s_ref, a_ref, s_out, a_out, sems):
    copies = [
        pltpu.make_async_copy(s_ref, s_out, sems.at[0]),
        pltpu.make_async_copy(a_ref, a_out, sems.at[1]),
    ]
    for copy in copies:
        copy.start()
    for copy in copies:
        copy.wait()


def feed_forcing():
    linear = -FEED_RATE
    return FEED_RATE * math.expm1(HALF_STEP * linear) / linear


def on_device(substrate, activator):
    wide, tall, turn1, turn2, down, across = constants()
    shape = pltpu.VMEM((COLS, 8, WIDE), F32)
    held = lambda x: pltpu.with_memory_space_constraint(x, pltpu.HBM)
    anywhere = pl.BlockSpec(memory_space=pltpu.HBM)
    vmem = lambda *shape: pltpu.VMEM(shape, F32)
    by_col, by_tile = (COLS, 8, WIDE), (TILES, 8, LANES)
    by_row = (ROWS, 8, LANES)
    half_col, half_row = (2, COLS, 8, LANES), (2, ROWS, 4, LANES)
    out = pl.pallas_call(
        kernel,
        name="section",
        out_shape=(shape, shape),
        in_specs=[anywhere] * 8,
        out_specs=(pl.BlockSpec(memory_space=pltpu.VMEM),) * 2,
        scratch_shapes=[
            vmem(3, *by_col),
            pltpu.VMEM(wide.shape, BF16),
            pltpu.VMEM(tall.shape, BF16),
            vmem(*turn1.shape),
            vmem(*turn2.shape),
            vmem(*down.shape),
            vmem(*across.shape),
            vmem(5, *by_tile),
            pltpu.VMEM(wide.shape, BF16),
            vmem(*by_col),
            vmem(*half_col),
            vmem(*half_col),
            vmem(*half_row),
            vmem(*half_row),
            vmem(*by_tile),
            vmem(2, *by_tile),
            vmem(2 * TILES, 8, LANES),
            vmem(2 * TILES, 8, 2 * LANES),
            vmem(*by_tile),
            vmem(2, *half_row),
            vmem(2, *half_row),
            vmem(2, *half_col),
            vmem(2, *half_col),
            vmem(2, *by_col),
            vmem(2, *by_row),
            vmem(2, *by_row),
            vmem(2, *by_row),
            vmem(2, *by_row),
            vmem(2, *by_col),
            vmem(2, *by_col),
            vmem(2, COLS // 2, 8, 2 * WIDE),
            pltpu.SemaphoreType.DMA((8,)),
            pltpu.SemaphoreType.DMA((21,)),
            pltpu.SemaphoreType.DMA((21,)),
        ],
        compiler_params=pltpu.CompilerParams(
            collective_id=0, has_side_effects=True, vmem_limit_bytes=20 << 20
        ),
    )(
        held(substrate.reshape(COLS, 8, WIDE)),
        held(activator.reshape(COLS, 8, WIDE)),
        held(jnp.asarray(wide)),
        held(jnp.asarray(tall)),
        held(jnp.asarray(turn1)),
        held(jnp.asarray(turn2)),
        held(jnp.asarray(down)),
        held(jnp.asarray(across)),
    )
    flat = jax.ShapeDtypeStruct(substrate.shape, F32)
    return pl.pallas_call(
        store_kernel,
        name="store",
        out_shape=(flat, flat),
        in_specs=[pl.BlockSpec(memory_space=pltpu.VMEM)] * 2,
        out_specs=(pl.BlockSpec(memory_space=pltpu.HBM),) * 2,
        scratch_shapes=[pltpu.SemaphoreType.DMA((2,))],
    )(*(pltpu.with_memory_space_constraint(x.reshape(substrate.shape), pltpu.VMEM) for x in out))


def solution(mesh):
    spec = P("row", "col")
    return jax.shard_map(
        on_device, mesh=mesh, in_specs=(spec, spec), out_specs=(spec, spec), check_vma=False
    )
```

```python
import math

import jax
import jax.numpy as jnp
import numpy as np
from jax import lax
from jax.experimental import pallas as pl
from jax.experimental.pallas import tpu as pltpu
from jax.sharding import PartitionSpec as P

FEED_RATE = 0.037
KILL_RATE = 0.06
HALF_STEP = 4.0
SUBSTRATE = (4e-07, FEED_RATE)
ACTIVATOR = (2e-07, FEED_RATE + KILL_RATE)
TOTAL = 4096
COLS = 16
ROWS = 32
WIDE = 256
LANES = 128
TILES = ROWS // 2
F32 = jnp.float32
BF16 = jnp.bfloat16


def c_add(a, b):
    im = a[1] if b[1] is None else (b[1] if a[1] is None else a[1] + b[1])
    return (a[0] + b[0], im)


def c_sub(a, b):
    im = a[1] if b[1] is None else (-b[1] if a[1] is None else a[1] - b[1])
    return (a[0] - b[0], im)


def c_conj(a):
    return (a[0], None if a[1] is None else -a[1])


def c_turn(a, numerator, denominator):
    numerator %= denominator
    if numerator == 0:
        return a
    if 4 * numerator == denominator:
        return (jnp.zeros_like(a[0]) if a[1] is None else -a[1], a[0])
    if 4 * numerator == 3 * denominator:
        return (jnp.zeros_like(a[0]) if a[1] is None else a[1], -a[0])
    cosine = math.cos(2.0 * math.pi * numerator / denominator)
    sine = math.sin(2.0 * math.pi * numerator / denominator)
    if a[1] is None:
        return (a[0] * cosine, a[0] * sine)
    return (a[0] * cosine - a[1] * sine, a[0] * sine + a[1] * cosine)


def real_forward(values):
    size = len(values)
    if size == 2:
        return [(values[0] + values[1], None), (values[0] - values[1], None)]
    even, odd = real_forward(values[::2]), real_forward(values[1::2])
    return join_halves(even, odd, size)


def join_halves(even, odd, size, first=0):
    half = size // 2
    out = [None] * (half + 1)
    for k in range(first, half // 2 + 1):
        turned = c_turn(odd[k], -k, size)
        out[k] = c_add(even[k], turned)
        if half - k != k:
            out[half - k] = c_conj(c_sub(even[k], turned))
    return out


def split_halves(spectrum, size, first=0):
    half = size // 2
    even, odd = [None] * (half // 2 + 1), [None] * (half // 2 + 1)
    for k in range(first, half // 2 + 1):
        if k == 0:
            even[k] = (spectrum[0][0] + spectrum[half][0], None)
            odd[k] = (spectrum[0][0] - spectrum[half][0], None)
        elif 2 * k == half:
            even[k] = (2.0 * spectrum[k][0], None)
            odd[k] = (-2.0 * spectrum[k][1], None)
        else:
            other = c_conj(spectrum[half - k])
            even[k] = c_add(spectrum[k], other)
            odd[k] = c_turn(c_sub(spectrum[k], other), k, size)
    return even, odd


def real_backward(spectrum):
    size = 2 * (len(spectrum) - 1)
    if size == 2:
        a, b = spectrum[0][0], spectrum[1][0]
        return [a + b, a - b]
    even, odd = split_halves(spectrum, size)
    even, odd = real_backward(even), real_backward(odd)
    return [x for pair in zip(even, odd) for x in pair]


def roll_rows(tile, shift):
    return pltpu.roll(tile, shift, 0)


def sublane():
    return lax.broadcasted_iota(jnp.int32, (8, LANES), 0)


def part_sign():
    return jnp.where(sublane() % 4 < 2, 1.0, -1.0).astype(F32)


def other_part(tile):
    return jnp.where(sublane() % 4 < 2, roll_rows(tile, 6), roll_rows(tile, 2))


def tile_turn(tile, cosine, signed_sine):
    return tile * cosine - signed_sine * other_part(tile)


def tile_fft(tiles, sign, direction):
    size = len(tiles)
    if size == 1:
        return tiles
    even, odd = tile_fft(tiles[::2], sign, direction), tile_fft(tiles[1::2], sign, direction)
    low, high = [], []
    for k in range(size // 2):
        turned = odd[k]
        if 4 * k == size:
            turned = (-direction * sign) * other_part(turned)
        elif k:
            angle = direction * 2.0 * math.pi * k / size
            turned = tile_turn(turned, math.cos(angle), sign * math.sin(angle))
        low.append(even[k] + turned)
        high.append(even[k] - turned)
    return low + high


def second_turn(tile, k, sign, direction):
    if k == 0:
        return tile
    angle = direction * 2.0 * math.pi * k / ROWS
    lower = sublane() < 4
    cosine = jnp.where(lower, 1.0, math.cos(angle)).astype(F32)
    sine = jnp.where(lower, 0.0, math.sin(angle)).astype(F32)
    return tile_turn(tile, cosine, sign * sine)


def block_sums(tile):
    return jnp.where(sublane() < 4, tile, -tile) + roll_rows(tile, 4)


def fft_down(tiles, sign):
    turned = [second_turn(x, k, sign, -1) for k, x in enumerate(tile_fft(tiles, sign, -1))]
    return [block_sums(x) for x in turned]


def fft_up(tiles, sign):
    turned = [second_turn(block_sums(x), k, sign, 1) for k, x in enumerate(tiles)]
    return tile_fft(turned, sign, 1)


MATRIX = (((1,), (0,)), ((), ()))


def pieces(values):
    top = values.astype(BF16)
    return top, (values - top.astype(F32)).astype(BF16)


def dot_wide(values, high, low):
    top, rest = pieces(values)
    size = values.shape[0]
    both = lax.dot_general(
        jnp.concatenate([top, rest], axis=0), high, MATRIX, preferred_element_type=F32
    )
    corner = lax.dot_general(top, low, MATRIX, preferred_element_type=F32)
    return both[:size] + (both[size:] + corner)


def dot_tall(values, matrix):
    top, rest = pieces(values)
    return lax.dot_general(
        jnp.concatenate([top, rest, top], axis=1), matrix, MATRIX, preferred_element_type=F32
    )


def forward_columns(values, turn_cos, turn_sin):
    even, odd = real_forward(values[::2]), real_forward(values[1::2])
    spectrum = join_halves(even, odd, COLS, 1)
    rows = [jnp.concatenate([even[0][0], odd[0][0]], axis=1)]
    for k in range(1, COLS // 2):
        re, im = spectrum[k]
        cosine, sine = turn_cos[k : k + 1, :], turn_sin[k : k + 1, :]
        rows.append(jnp.concatenate([re * cosine + im * sine, im * cosine - re * sine], axis=1))
    return jnp.concatenate(rows, axis=0)


def half_product(stacked, weights):
    out = dot_wide(stacked, weights[0], weights[1])
    first = dot_wide(stacked[:16], weights[2], weights[3])
    return [first[:8]] + [out[8 * slot : 8 * slot + 8] for slot in range(1, COLS // 2)]


def backward_columns(products, turn_cos, turn_sin):
    spectrum = [None] * (COLS // 2)
    for k in range(1, COLS // 2):
        re, im = products[k][:, :WIDE], products[k][:, WIDE:]
        cosine, sine = turn_cos[k : k + 1, :], turn_sin[k : k + 1, :]
        spectrum[k] = (re * cosine - im * sine, im * cosine + re * sine)
    even, odd = split_halves(spectrum + [None], COLS, 1)
    even[0], odd[0] = (products[0][:, :WIDE], None), (products[0][:, WIDE:], None)
    even, odd = real_backward(even), real_backward(odd)
    return [x for pair in zip(even, odd) for x in pair]


def squared_wave(index):
    signed = jnp.where(2 * index < TOTAL, index, index - TOTAL).astype(F32)
    angular = (2.0 * math.pi) * signed
    return angular * angular


def forcing_of(wave_number, diffusion, decay_rate):
    linear = -diffusion * wave_number - decay_rate
    return (jnp.exp(HALF_STEP * linear) - 1.0) / linear


def forcings(step, half, row, col):
    column = sublane() % 2
    slot, side = col // 2, col % 2
    within = LANES * side + 4 * row + 2 * half + column
    q = jnp.where(slot == 0, 8 * within, slot + COLS * within)
    p = step + TILES * (sublane() // 4) + ROWS * lax.broadcasted_iota(jnp.int32, (8, LANES), 1)
    row_wave = squared_wave(p)
    wave_number = row_wave + squared_wave(q)
    norm = 1.0 / (TOTAL * TOTAL)
    scale = jnp.where(q == 0, norm, jnp.where(slot == 0, 2.0 * norm, norm)).astype(F32)
    out = [
        -scale * forcing_of(wave_number, *SUBSTRATE),
        scale * forcing_of(wave_number, *ACTIVATOR),
    ]
    if half == 0:
        last = row_wave + (2.0 * math.pi * (TOTAL // 2)) ** 2
        first = -norm * forcing_of(last, *SUBSTRATE)
        out.append(jnp.where(column == 0, first, norm * forcing_of(last, *ACTIVATOR)))
    return out


def column_growth(index, diffusion):
    angular = 2.0 * np.pi * np.where(2 * index < TOTAL, index, index - TOTAL)
    return np.exp(-HALF_STEP * diffusion * angular * angular)


def constants():
    def split(matrix):
        high = matrix.astype(np.float32).astype(BF16)
        return high, (matrix - high.astype(np.float64)).astype(np.float32).astype(BF16)

    def interleave(re, im):
        both = np.stack([re, im], axis=1).reshape(-1, 2, 2, ROWS, 2, 2)
        return both.transpose(0, 4, 2, 3, 1, 5).reshape(re.shape[0], -1)

    j = np.arange(WIDE)
    angle = 2.0 * np.pi * (np.outer(j, j) % WIDE) / WIDE
    cos, sin = np.cos(angle), np.sin(angle)
    pair = interleave(np.concatenate([cos, sin]), np.concatenate([-sin, cos]))
    long = np.arange(2 * WIDE)
    angle = 2.0 * np.pi * (np.outer(long, j) % (2 * WIDE)) / (2 * WIDE)
    cos, sin = np.cos(angle), -np.sin(angle)
    sin[:, 0] = 1.0 - 2.0 * (long % 2)
    single = interleave(cos, sin)
    wide = np.stack([*split(pair), *split(single)])
    i = np.arange(LANES)
    angle = 2.0 * np.pi * (np.outer(i, i) % LANES) / LANES
    high, low = split(np.concatenate([np.cos(angle), np.sin(angle)], axis=1))
    tall = np.concatenate([high, high, low])

    angle = 2.0 * np.pi * np.outer(np.arange(COLS // 2), j) / TOTAL
    turn1 = np.stack([np.cos(angle), np.sin(angle)]).astype(np.float32)
    block, part, _ = np.unravel_index(np.arange(8), (2, 2, 2))
    wave = np.arange(TILES)[:, None] + TILES * block
    angle = 2.0 * np.pi * wave[:, :, None] * i / TOTAL
    sign = np.where(part == 0, 1.0, -1.0)[:, None]
    turn2 = np.stack([np.cos(angle), sign * np.sin(angle)]).astype(np.float32)
    rows = np.arange(ROWS)[:, None] + ROWS * i
    angle = 2.0 * np.pi * np.arange(ROWS)[:, None] * i / TOTAL
    down = [np.cos(angle), np.sin(angle)]
    slot = np.arange(COLS // 2)[:, None]
    q = np.where(slot == 0, 8 * j, slot + COLS * j)
    last = np.where(q == 0, TOTAL // 2, q)
    paired = np.where(slot == 0, 2.0, 1.0)
    across = []
    for diffusion, decay_rate in (SUBSTRATE, ACTIVATOR):
        down.append(column_growth(rows, diffusion) / TOTAL)
        decay = math.exp(-HALF_STEP * decay_rate) / TOTAL
        parts = [
            np.where(q == 0, 1.0, paired) * column_growth(waves, diffusion) * decay
            for waves in (q, last)
        ]
        across.append(interleave(*parts))
    down, across = np.stack(down).astype(np.float32), np.stack(across).astype(np.float32)
    return wide, tall, turn1, turn2, down, across


SEND1, SEND2, SEND3, SEND4, SEND5, SEND6 = 0, 1, 3, 5, 9, 13
SENDA, SENDB, SENDC = 15, 17, 19


def kernel(
    u_hbm, v_hbm, wide_hbm, tall_hbm, turn1_hbm, turn2_hbm, down_hbm, across_hbm, s_out, a_out,
    fields, wide, tall, turn1, turn2, down, across, tables, back,
    got1, put2, got2, put3, got3, tiles, spectra, pair, products, extra,
    put4, got4, put5, got5, put6,
    put_a, got_a, put_b, got_b, put_c, got_c, grown, partial, local_sem, send_sem, recv_sem,
):
    row, col = lax.axis_index("row"), lax.axis_index("col")
    mesh_id = pl.DeviceIdType.MESH

    loads = [
        pltpu.make_async_copy(src, dst, local_sem.at[n])
        for n, (src, dst) in enumerate(
            [
                (u_hbm, fields.at[0]),
                (v_hbm, fields.at[1]),
                (wide_hbm, wide),
                (tall_hbm, tall),
                (turn1_hbm, turn1),
                (turn2_hbm, turn2),
                (down_hbm, down),
                (across_hbm, across),
            ]
        )
    ]
    for load in loads:
        load.start()

    barrier = pltpu.get_barrier_semaphore()

    def greet(axis, me, size):
        def body(peer, carry):
            pl.semaphore_signal(barrier, inc=1, device_id={axis: peer}, device_id_type=mesh_id)
            return carry

        lax.fori_loop(me + 1, size, body, 0)
        lax.fori_loop(0, me, body, 0)

    pending = []

    def piece(axis, peer, source, target, sem):
        return pltpu.make_async_remote_copy(
            src_ref=source,
            dst_ref=target,
            send_sem=send_sem.at[sem],
            recv_sem=recv_sem.at[sem],
            device_id={axis: peer},
            device_id_type=mesh_id,
        )

    def send(axis, source, target, sem):
        me, size = (col, COLS) if axis == "col" else (row, ROWS)

        def body(peer, carry):
            piece(axis, peer, source.at[peer], target.at[me], sem).start()
            return carry

        lax.fori_loop(me + 1, size, body, 0)
        lax.fori_loop(0, me, body, 0)
        pending.append((axis, source, sem))

    def whole(axis, block, sem):
        me, size = (col, COLS) if axis == "col" else (row, ROWS)
        block = block.at[pl.ds(0, size - 1)]
        return piece(axis, lax.rem(me + 1, size), block, block, sem)

    greet("col", col, COLS)
    greet("row", row, ROWS)
    loads[0].wait()
    loads[1].wait()
    fields[2] = fields[0] * fields[1] * fields[1]
    pl.semaphore_wait(barrier, COLS - 1 + ROWS - 1)

    sign = part_sign()

    send("col", fields.at[2], got1, SEND1)
    got1[col] = fields[2, col]

    for n in range(2):
        put_a[n] = fields[n].reshape(LANES, WIDE).T.reshape(ROWS, 8, LANES)
        send("row", put_a.at[n], got_a.at[n], SENDA + n)
        got_a[n, row] = put_a[n, row]

    def fill(step, carry):
        for half in range(2):
            for n, table in enumerate(forcings(step, half, row, col)):
                tables[3 * half + n, step] = table
        return carry

    lax.fori_loop(0, TILES, fill, 0)
    for load in loads[2:]:
        load.wait()

    def spectrum_of(values, keep):
        stacked = forward_columns(values, turn1[0], turn1[1])
        for h in range(2):
            part = pl.ds(WIDE * h, WIDE)
            keep(h, half_product(stacked, [wide[k, :, part] for k in range(4)]))

    whole("col", got1, SEND1).wait_recv()
    def send_half(h, rows):
        for c in range(COLS):
            start = LANES * (c % 2)
            put2[h, c] = rows[c // 2][:, start : start + LANES]
        send("col", put2.at[h], got2.at[h], SEND2 + h)
        got2[h, col] = put2[h, col]

    spectrum_of([got1[c] for c in range(COLS)], send_half)

    def filter_columns(n):
        whole("row", got_a.at[n], SENDA + n).wait_recv()
        values = tile_fft([got_a[n, r] for r in range(ROWS)], sign, -1)
        for k in range(ROWS):
            cosine, sine = down[0, k : k + 1, :], sign * down[1, k : k + 1, :]
            pair[k] = tile_turn(values[k], cosine, -sine)
        out = dot_tall(pair[...].reshape(ROWS * 8, LANES), tall[...])
        products[pl.ds(0, ROWS)] = out.reshape(ROWS, 8, 2 * LANES)
        for k in range(ROWS):
            both = products[k]
            wave = both[:, :LANES] + sign * other_part(both[:, LANES:])
            pair[k] = wave * down[2 + n, k : k + 1, :]
        out = dot_tall(pair[...].reshape(ROWS * 8, LANES), tall[...])
        products[pl.ds(0, ROWS)] = out.reshape(ROWS, 8, 2 * LANES)
        turned = []
        for k in range(ROWS):
            both = products[k]
            tile = both[:, :LANES] - sign * other_part(both[:, LANES:])
            cosine, sine = down[0, k : k + 1, :], sign * down[1, k : k + 1, :]
            turned.append(tile_turn(tile, cosine, sine))
        values = tile_fft(turned, sign, 1)
        for r in range(ROWS):
            put_b[n, r] = values[r]
        send("row", put_b.at[n], got_b.at[n], SENDB + n)
        got_b[n, row] = put_b[n, row]

    def send_rows(n):
        whole("row", got_b.at[n], SENDB + n).wait_recv()
        put_c[n] = got_b[n].reshape(WIDE, LANES).T.reshape(COLS, 8, WIDE)
        send("col", put_c.at[n], got_c.at[n], SENDC + n)
        got_c[n, col] = put_c[n, col]

    def grow(n):
        whole("col", got_c.at[n], SENDC + n).wait_recv()
        def keep(h, rows):
            part = pl.ds(WIDE * h, WIDE)
            for s in range(COLS // 2):
                grown[n, h, s] = rows[s] * across[n, s : s + 1, part]

        spectrum_of([got_c[n, c] for c in range(COLS)], keep)

    def turn_columns(h):
        whole("col", got2.at[h], SEND2 + h).wait_recv()
        turned = got2[h].reshape(LANES, LANES).T
        for r in range(ROWS):
            put3[h, r] = turned[4 * r : 4 * r + 4]
        send("row", put3.at[h], got3.at[h], SEND3 + h)
        got3[h, row] = put3[h, row]

    def two_blocks(ref, t):
        return jnp.concatenate([ref[2 * t], ref[2 * t + 1]], axis=0)

    def forward_down(h):
        whole("row", got3.at[h], SEND3 + h).wait_recv()
        values = fft_down([two_blocks(got3.at[h], t) for t in range(TILES)], sign)
        for k in range(TILES):
            tiles[k] = tile_turn(values[k], turn2[0, k], -turn2[1, k])
        out = dot_tall(tiles[...].reshape(LANES, LANES), tall[...])
        products[pl.ds(0, TILES)] = out.reshape(TILES, 8, 2 * LANES)
        for k in range(TILES):
            both = products[k]
            spectra[h, k] = both[:, :LANES] + sign * other_part(both[:, LANES:])

    special = sublane() % 4 == jnp.where(row + col == 0, 2, -1)

    def backward_down(n, h):
        parts = 2 if n == 0 and h == 0 else 1
        for k in range(TILES):
            wave = spectra[h, k]
            pair[k] = tables[3 * h + n, k] * wave
            if parts == 2:
                both = jnp.where(sublane() % 2 == 0, wave, roll_rows(wave, 1))
                pair[TILES + k] = tables[2, k] * both
        block = pair[pl.ds(0, parts * TILES)].reshape(parts * LANES, LANES)
        out = dot_tall(block, tall[...])
        products[pl.ds(0, parts * TILES)] = out.reshape(parts * TILES, 8, 2 * LANES)
        for m in reversed(range(parts)):
            turned = []
            for k in range(TILES):
                both = products[m * TILES + k]
                tile = both[:, :LANES] - sign * other_part(both[:, LANES:])
                turned.append(tile_turn(tile, turn2[0, k], turn2[1, k]))
            values = fft_up(turned, sign)
            for t in range(TILES):
                value = values[t]
                if m == 1:
                    extra[t] = value
                    continue
                if h == 0:
                    fixed = extra[t] if n == 0 else roll_rows(extra[t], 7)
                    value = jnp.where(special, fixed, value)
                put4[n, h, 2 * t] = value[:4]
                put4[n, h, 2 * t + 1] = value[4:]
        send("row", put4.at[n, h], got4.at[n, h], SEND4 + 2 * n + h)
        got4[n, h, row] = put4[n, h, row]

    def turn_back(n, h):
        whole("row", got4.at[n, h], SEND4 + 2 * n + h).wait_recv()
        block = jnp.concatenate([two_blocks(got4.at[n, h], t) for t in range(TILES)], axis=0)
        put5[n, h] = block.T.reshape(COLS, 8, LANES)
        send("col", put5.at[n, h], got5.at[n, h], SEND5 + 2 * n + h)
        got5[n, h, col] = put5[n, h, col]

    filter_columns(0)
    for k in range(4):
        back[k] = wide.at[k][...].T
    turn_columns(0)
    turn_columns(1)
    filter_columns(1)
    send_rows(0)
    forward_down(0)
    backward_down(0, 0)
    forward_down(1)
    backward_down(0, 1)
    send_rows(1)
    backward_down(1, 0)
    backward_down(1, 1)
    grow(0)
    for n in range(2):
        for h in range(2):
            turn_back(n, h)
    grow(1)

    feed = feed_forcing()
    for n, out in enumerate((s_out, a_out)):
        for h in range(2):
            whole("col", got5.at[n, h], SEND5 + 2 * n + h).wait_recv()
            rows = [
                jnp.concatenate([got5[n, h, 2 * s], got5[n, h, 2 * s + 1]], axis=1) + grown[n, h, s]
                for s in range(COLS // 2)
            ]
            weights = [back[k, pl.ds(WIDE * h, WIDE), :] for k in range(4)]
            rows = half_product(jnp.concatenate(rows, axis=0), weights)
            if h == 0:
                for s in range(COLS // 2):
                    partial[s] = rows[s]
            else:
                for s in range(COLS // 2):
                    partial[s] = partial[s] + rows[s]
        total = [partial[s] for s in range(COLS // 2)]
        values = backward_columns(total, turn1[0], turn1[1])
        for c in range(COLS):
            put6[n, c] = values[c] + feed if n == 0 else values[c]
        send("col", put6.at[n], out, SEND6 + n)
        out[col] = put6[n, col]

    for n, out in enumerate((s_out, a_out)):
        whole("col", out, SEND6 + n).wait_recv()
    for entry in pending:
        whole(*entry).wait_send()


def store_kernel(s_ref, a_ref, s_out, a_out, sems):
    copies = [
        pltpu.make_async_copy(s_ref, s_out, sems.at[0]),
        pltpu.make_async_copy(a_ref, a_out, sems.at[1]),
    ]
    for copy in copies:
        copy.start()
    for copy in copies:
        copy.wait()


def feed_forcing():
    linear = -FEED_RATE
    return FEED_RATE * math.expm1(HALF_STEP * linear) / linear


def on_device(substrate, activator):
    wide, tall, turn1, turn2, down, across = constants()
    shape = pltpu.VMEM((COLS, 8, WIDE), F32)
    held = lambda x: pltpu.with_memory_space_constraint(x, pltpu.HBM)
    anywhere = pl.BlockSpec(memory_space=pltpu.HBM)
    vmem = lambda *shape: pltpu.VMEM(shape, F32)
    by_col, by_tile = (COLS, 8, WIDE), (TILES, 8, LANES)
    by_row = (ROWS, 8, LANES)
    half_col, half_row = (2, COLS, 8, LANES), (2, ROWS, 4, LANES)
    out = pl.pallas_call(
        kernel,
        name="section",
        out_shape=(shape, shape),
        in_specs=[anywhere] * 8,
        out_specs=(pl.BlockSpec(memory_space=pltpu.VMEM),) * 2,
        scratch_shapes=[
            vmem(3, *by_col),
            pltpu.VMEM(wide.shape, BF16),
            pltpu.VMEM(tall.shape, BF16),
            vmem(*turn1.shape),
            vmem(*turn2.shape),
            vmem(*down.shape),
            vmem(*across.shape),
            vmem(5, *by_tile),
            pltpu.VMEM(wide.shape, BF16),
            vmem(*by_col),
            vmem(*half_col),
            vmem(*half_col),
            vmem(*half_row),
            vmem(*half_row),
            vmem(*by_tile),
            vmem(2, *by_tile),
            vmem(2 * TILES, 8, LANES),
            vmem(2 * TILES, 8, 2 * LANES),
            vmem(*by_tile),
            vmem(2, *half_row),
            vmem(2, *half_row),
            vmem(2, *half_col),
            vmem(2, *half_col),
            vmem(2, *by_col),
            vmem(2, *by_row),
            vmem(2, *by_row),
            vmem(2, *by_row),
            vmem(2, *by_row),
            vmem(2, *by_col),
            vmem(2, *by_col),
            vmem(2, 2, COLS // 2, 8, WIDE),
            vmem(COLS // 2, 8, 2 * WIDE),
            pltpu.SemaphoreType.DMA((8,)),
            pltpu.SemaphoreType.DMA((21,)),
            pltpu.SemaphoreType.DMA((21,)),
        ],
        compiler_params=pltpu.CompilerParams(
            collective_id=0, has_side_effects=True, vmem_limit_bytes=20 << 20
        ),
    )(
        held(substrate.reshape(COLS, 8, WIDE)),
        held(activator.reshape(COLS, 8, WIDE)),
        held(jnp.asarray(wide)),
        held(jnp.asarray(tall)),
        held(jnp.asarray(turn1)),
        held(jnp.asarray(turn2)),
        held(jnp.asarray(down)),
        held(jnp.asarray(across)),
    )
    flat = jax.ShapeDtypeStruct(substrate.shape, F32)
    return pl.pallas_call(
        store_kernel,
        name="store",
        out_shape=(flat, flat),
        in_specs=[pl.BlockSpec(memory_space=pltpu.VMEM)] * 2,
        out_specs=(pl.BlockSpec(memory_space=pltpu.HBM),) * 2,
        scratch_shapes=[pltpu.SemaphoreType.DMA((2,))],
    )(*(pltpu.with_memory_space_constraint(x.reshape(substrate.shape), pltpu.VMEM) for x in out))


def solution(mesh):
    spec = P("row", "col")
    return jax.shard_map(
        on_device, mesh=mesh, in_specs=(spec, spec), out_specs=(spec, spec), check_vma=False
    )
```

```python
import math

import jax
import jax.numpy as jnp
import numpy as np
from jax import lax
from jax.experimental import pallas as pl
from jax.experimental.pallas import tpu as pltpu
from jax.sharding import PartitionSpec as P

FEED_RATE = 0.037
KILL_RATE = 0.06
HALF_STEP = 4.0
SUBSTRATE = (4e-07, FEED_RATE)
ACTIVATOR = (2e-07, FEED_RATE + KILL_RATE)
TOTAL = 4096
COLS = 16
ROWS = 32
WIDE = 256
LANES = 128
TILES = ROWS // 2
F32 = jnp.float32
BF16 = jnp.bfloat16


def c_add(a, b):
    im = a[1] if b[1] is None else (b[1] if a[1] is None else a[1] + b[1])
    return (a[0] + b[0], im)


def c_sub(a, b):
    im = a[1] if b[1] is None else (-b[1] if a[1] is None else a[1] - b[1])
    return (a[0] - b[0], im)


def c_conj(a):
    return (a[0], None if a[1] is None else -a[1])


def c_turn(a, numerator, denominator):
    numerator %= denominator
    if numerator == 0:
        return a
    if 4 * numerator == denominator:
        return (jnp.zeros_like(a[0]) if a[1] is None else -a[1], a[0])
    if 4 * numerator == 3 * denominator:
        return (jnp.zeros_like(a[0]) if a[1] is None else a[1], -a[0])
    cosine = math.cos(2.0 * math.pi * numerator / denominator)
    sine = math.sin(2.0 * math.pi * numerator / denominator)
    if a[1] is None:
        return (a[0] * cosine, a[0] * sine)
    return (a[0] * cosine - a[1] * sine, a[0] * sine + a[1] * cosine)


def real_forward(values):
    size = len(values)
    if size == 2:
        return [(values[0] + values[1], None), (values[0] - values[1], None)]
    even, odd = real_forward(values[::2]), real_forward(values[1::2])
    return join_halves(even, odd, size)


def join_halves(even, odd, size, first=0):
    half = size // 2
    out = [None] * (half + 1)
    for k in range(first, half // 2 + 1):
        turned = c_turn(odd[k], -k, size)
        out[k] = c_add(even[k], turned)
        if half - k != k:
            out[half - k] = c_conj(c_sub(even[k], turned))
    return out


def split_halves(spectrum, size, first=0):
    half = size // 2
    even, odd = [None] * (half // 2 + 1), [None] * (half // 2 + 1)
    for k in range(first, half // 2 + 1):
        if k == 0:
            even[k] = (spectrum[0][0] + spectrum[half][0], None)
            odd[k] = (spectrum[0][0] - spectrum[half][0], None)
        elif 2 * k == half:
            even[k] = (2.0 * spectrum[k][0], None)
            odd[k] = (-2.0 * spectrum[k][1], None)
        else:
            other = c_conj(spectrum[half - k])
            even[k] = c_add(spectrum[k], other)
            odd[k] = c_turn(c_sub(spectrum[k], other), k, size)
    return even, odd


def real_backward(spectrum):
    size = 2 * (len(spectrum) - 1)
    if size == 2:
        a, b = spectrum[0][0], spectrum[1][0]
        return [a + b, a - b]
    even, odd = split_halves(spectrum, size)
    even, odd = real_backward(even), real_backward(odd)
    return [x for pair in zip(even, odd) for x in pair]


def roll_rows(tile, shift):
    return pltpu.roll(tile, shift, 0)


def sublane():
    return lax.broadcasted_iota(jnp.int32, (8, LANES), 0)


def part_sign():
    return jnp.where(sublane() % 4 < 2, 1.0, -1.0).astype(F32)


def other_part(tile):
    return jnp.where(sublane() % 4 < 2, roll_rows(tile, 6), roll_rows(tile, 2))


def tile_turn(tile, cosine, signed_sine):
    return tile * cosine - signed_sine * other_part(tile)


def tile_fft(tiles, sign, direction):
    size = len(tiles)
    if size == 1:
        return tiles
    even, odd = tile_fft(tiles[::2], sign, direction), tile_fft(tiles[1::2], sign, direction)
    low, high = [], []
    for k in range(size // 2):
        turned = odd[k]
        if 4 * k == size:
            turned = (-direction * sign) * other_part(turned)
        elif k:
            angle = direction * 2.0 * math.pi * k / size
            turned = tile_turn(turned, math.cos(angle), sign * math.sin(angle))
        low.append(even[k] + turned)
        high.append(even[k] - turned)
    return low + high


def second_turn(tile, k, sign, direction):
    if k == 0:
        return tile
    angle = direction * 2.0 * math.pi * k / ROWS
    lower = sublane() < 4
    cosine = jnp.where(lower, 1.0, math.cos(angle)).astype(F32)
    sine = jnp.where(lower, 0.0, math.sin(angle)).astype(F32)
    return tile_turn(tile, cosine, sign * sine)


def block_sums(tile):
    return jnp.where(sublane() < 4, tile, -tile) + roll_rows(tile, 4)


def fft_down(tiles, sign):
    turned = [second_turn(x, k, sign, -1) for k, x in enumerate(tile_fft(tiles, sign, -1))]
    return [block_sums(x) for x in turned]


def fft_up(tiles, sign):
    turned = [second_turn(block_sums(x), k, sign, 1) for k, x in enumerate(tiles)]
    return tile_fft(turned, sign, 1)


MATRIX = (((1,), (0,)), ((), ()))


def pieces(values):
    top = values.astype(BF16)
    return top, (values - top.astype(F32)).astype(BF16)


def dot_wide(values, high, low):
    top, rest = pieces(values)
    size = values.shape[0]
    both = lax.dot_general(
        jnp.concatenate([top, rest], axis=0), high, MATRIX, preferred_element_type=F32
    )
    corner = lax.dot_general(top, low, MATRIX, preferred_element_type=F32)
    return both[:size] + (both[size:] + corner)


def dot_tall(values, matrix):
    top, rest = pieces(values)
    stacked = jnp.concatenate([top, rest, top], axis=1)
    parts = [
        lax.dot_general(stacked, part, MATRIX, preferred_element_type=F32)
        for part in (matrix[:, :LANES], matrix[:, LANES:])
    ]
    return jnp.concatenate(parts, axis=1)


def forward_columns(values, turn_cos, turn_sin):
    even, odd = real_forward(values[::2]), real_forward(values[1::2])
    spectrum = join_halves(even, odd, COLS, 1)
    rows = [jnp.concatenate([even[0][0], odd[0][0]], axis=1)]
    for k in range(1, COLS // 2):
        re, im = spectrum[k]
        cosine, sine = turn_cos[k : k + 1, :], turn_sin[k : k + 1, :]
        rows.append(jnp.concatenate([re * cosine + im * sine, im * cosine - re * sine], axis=1))
    return jnp.concatenate(rows, axis=0)


def half_product(stacked, weights):
    out = dot_wide(stacked, weights[0], weights[1])
    first = dot_wide(stacked[:16], weights[2], weights[3])
    return [first[:8]] + [out[8 * slot : 8 * slot + 8] for slot in range(1, COLS // 2)]


def backward_columns(products, turn_cos, turn_sin):
    spectrum = [None] * (COLS // 2)
    for k in range(1, COLS // 2):
        re, im = products[k][:, :WIDE], products[k][:, WIDE:]
        cosine, sine = turn_cos[k : k + 1, :], turn_sin[k : k + 1, :]
        spectrum[k] = (re * cosine - im * sine, im * cosine + re * sine)
    even, odd = split_halves(spectrum + [None], COLS, 1)
    even[0], odd[0] = (products[0][:, :WIDE], None), (products[0][:, WIDE:], None)
    even, odd = real_backward(even), real_backward(odd)
    return [x for pair in zip(even, odd) for x in pair]


def squared_wave(index):
    signed = jnp.where(2 * index < TOTAL, index, index - TOTAL).astype(F32)
    angular = (2.0 * math.pi) * signed
    return angular * angular


def forcing_of(wave_number, diffusion, decay_rate):
    linear = -diffusion * wave_number - decay_rate
    return (jnp.exp(HALF_STEP * linear) - 1.0) / linear


def forcings(step, half, row, col):
    column = sublane() % 2
    slot, side = col // 2, col % 2
    within = LANES * side + 4 * row + 2 * half + column
    q = jnp.where(slot == 0, 8 * within, slot + COLS * within)
    p = step + TILES * (sublane() // 4) + ROWS * lax.broadcasted_iota(jnp.int32, (8, LANES), 1)
    row_wave = squared_wave(p)
    wave_number = row_wave + squared_wave(q)
    norm = 1.0 / (TOTAL * TOTAL)
    scale = jnp.where(q == 0, norm, jnp.where(slot == 0, 2.0 * norm, norm)).astype(F32)
    out = [
        -scale * forcing_of(wave_number, *SUBSTRATE),
        scale * forcing_of(wave_number, *ACTIVATOR),
    ]
    if half == 0:
        last = row_wave + (2.0 * math.pi * (TOTAL // 2)) ** 2
        first = -norm * forcing_of(last, *SUBSTRATE)
        out.append(jnp.where(column == 0, first, norm * forcing_of(last, *ACTIVATOR)))
    return out


def column_growth(index, diffusion):
    angular = 2.0 * np.pi * np.where(2 * index < TOTAL, index, index - TOTAL)
    return np.exp(-HALF_STEP * diffusion * angular * angular)


def constants():
    def split(matrix):
        high = matrix.astype(np.float32).astype(BF16)
        return high, (matrix - high.astype(np.float64)).astype(np.float32).astype(BF16)

    def interleave(re, im):
        both = np.stack([re, im], axis=1).reshape(-1, 2, 2, ROWS, 2, 2)
        return both.transpose(0, 4, 2, 3, 1, 5).reshape(re.shape[0], -1)

    j = np.arange(WIDE)
    angle = 2.0 * np.pi * (np.outer(j, j) % WIDE) / WIDE
    cos, sin = np.cos(angle), np.sin(angle)
    pair = interleave(np.concatenate([cos, sin]), np.concatenate([-sin, cos]))
    long = np.arange(2 * WIDE)
    angle = 2.0 * np.pi * (np.outer(long, j) % (2 * WIDE)) / (2 * WIDE)
    cos, sin = np.cos(angle), -np.sin(angle)
    sin[:, 0] = 1.0 - 2.0 * (long % 2)
    single = interleave(cos, sin)
    wide = np.stack([*split(pair), *split(single)])
    i = np.arange(LANES)
    angle = 2.0 * np.pi * (np.outer(i, i) % LANES) / LANES
    high, low = split(np.concatenate([np.cos(angle), np.sin(angle)], axis=1))
    tall = np.concatenate([high, high, low])

    angle = 2.0 * np.pi * np.outer(np.arange(COLS // 2), j) / TOTAL
    turn1 = np.stack([np.cos(angle), np.sin(angle)]).astype(np.float32)
    block, part, _ = np.unravel_index(np.arange(8), (2, 2, 2))
    wave = np.arange(TILES)[:, None] + TILES * block
    angle = 2.0 * np.pi * wave[:, :, None] * i / TOTAL
    sign = np.where(part == 0, 1.0, -1.0)[:, None]
    turn2 = np.stack([np.cos(angle), sign * np.sin(angle)]).astype(np.float32)
    rows = np.arange(ROWS)[:, None] + ROWS * i
    angle = 2.0 * np.pi * np.arange(ROWS)[:, None] * i / TOTAL
    down = [np.cos(angle), np.sin(angle)]
    slot = np.arange(COLS // 2)[:, None]
    q = np.where(slot == 0, 8 * j, slot + COLS * j)
    last = np.where(q == 0, TOTAL // 2, q)
    paired = np.where(slot == 0, 2.0, 1.0)
    across = []
    for diffusion, decay_rate in (SUBSTRATE, ACTIVATOR):
        down.append(column_growth(rows, diffusion) / TOTAL)
        decay = math.exp(-HALF_STEP * decay_rate) / TOTAL
        parts = [
            np.where(q == 0, 1.0, paired) * column_growth(waves, diffusion) * decay
            for waves in (q, last)
        ]
        across.append(interleave(*parts))
    down, across = np.stack(down).astype(np.float32), np.stack(across).astype(np.float32)
    return wide, tall, turn1, turn2, down, across


SEND1, SEND2, SEND3, SEND4, SEND5, SEND6 = 0, 1, 3, 5, 9, 13
SENDA, SENDB, SENDC = 15, 17, 19


def kernel(
    u_hbm, v_hbm, wide_hbm, tall_hbm, turn1_hbm, turn2_hbm, down_hbm, across_hbm, s_out, a_out,
    fields, wide, tall, turn1, turn2, down, across, tables, back,
    got1, put2, got2, put3, got3, tiles, spectra, pair, products, extra,
    put4, got4, put5, got5, put6,
    put_a, got_a, put_b, got_b, put_c, got_c, grown, partial, local_sem, send_sem, recv_sem,
):
    row, col = lax.axis_index("row"), lax.axis_index("col")
    mesh_id = pl.DeviceIdType.MESH

    loads = [
        pltpu.make_async_copy(src, dst, local_sem.at[n])
        for n, (src, dst) in enumerate(
            [
                (u_hbm, fields.at[0]),
                (v_hbm, fields.at[1]),
                (wide_hbm, wide),
                (tall_hbm, tall),
                (turn1_hbm, turn1),
                (turn2_hbm, turn2),
                (down_hbm, down),
                (across_hbm, across),
            ]
        )
    ]
    for load in loads:
        load.start()

    barrier = pltpu.get_barrier_semaphore()

    def greet(axis, me, size):
        def body(peer, carry):
            pl.semaphore_signal(barrier, inc=1, device_id={axis: peer}, device_id_type=mesh_id)
            return carry

        lax.fori_loop(me + 1, size, body, 0)
        lax.fori_loop(0, me, body, 0)

    pending = []

    def piece(axis, peer, source, target, sem):
        return pltpu.make_async_remote_copy(
            src_ref=source,
            dst_ref=target,
            send_sem=send_sem.at[sem],
            recv_sem=recv_sem.at[sem],
            device_id={axis: peer},
            device_id_type=mesh_id,
        )

    def send(axis, source, target, sem):
        me, size = (col, COLS) if axis == "col" else (row, ROWS)

        def body(peer, carry):
            piece(axis, peer, source.at[peer], target.at[me], sem).start()
            return carry

        lax.fori_loop(me + 1, size, body, 0)
        lax.fori_loop(0, me, body, 0)
        pending.append((axis, source, sem))

    def whole(axis, block, sem):
        me, size = (col, COLS) if axis == "col" else (row, ROWS)
        block = block.at[pl.ds(0, size - 1)]
        return piece(axis, lax.rem(me + 1, size), block, block, sem)

    greet("col", col, COLS)
    greet("row", row, ROWS)
    loads[0].wait()
    loads[1].wait()
    fields[2] = fields[0] * fields[1] * fields[1]
    pl.semaphore_wait(barrier, COLS - 1 + ROWS - 1)

    sign = part_sign()

    send("col", fields.at[2], got1, SEND1)
    got1[col] = fields[2, col]

    for n in range(2):
        put_a[n] = fields[n].reshape(LANES, WIDE).T.reshape(ROWS, 8, LANES)
        send("row", put_a.at[n], got_a.at[n], SENDA + n)
        got_a[n, row] = put_a[n, row]

    def fill(step, carry):
        for half in range(2):
            for n, table in enumerate(forcings(step, half, row, col)):
                tables[3 * half + n, step] = table
        return carry

    lax.fori_loop(0, TILES, fill, 0)
    for load in loads[2:]:
        load.wait()

    def spectrum_of(values, keep):
        stacked = forward_columns(values, turn1[0], turn1[1])
        for h in range(2):
            part = pl.ds(WIDE * h, WIDE)
            keep(h, half_product(stacked, [wide[k, :, part] for k in range(4)]))

    whole("col", got1, SEND1).wait_recv()
    def send_half(h, rows):
        for c in range(COLS):
            start = LANES * (c % 2)
            put2[h, c] = rows[c // 2][:, start : start + LANES]
        send("col", put2.at[h], got2.at[h], SEND2 + h)
        got2[h, col] = put2[h, col]

    spectrum_of([got1[c] for c in range(COLS)], send_half)

    def filter_columns(n):
        whole("row", got_a.at[n], SENDA + n).wait_recv()
        values = tile_fft([got_a[n, r] for r in range(ROWS)], sign, -1)
        for k in range(ROWS):
            cosine, sine = down[0, k : k + 1, :], sign * down[1, k : k + 1, :]
            pair[k] = tile_turn(values[k], cosine, -sine)
        out = dot_tall(pair[...].reshape(ROWS * 8, LANES), tall[...])
        products[pl.ds(0, ROWS)] = out.reshape(ROWS, 8, 2 * LANES)
        for k in range(ROWS):
            both = products[k]
            wave = both[:, :LANES] + sign * other_part(both[:, LANES:])
            pair[k] = wave * down[2 + n, k : k + 1, :]
        out = dot_tall(pair[...].reshape(ROWS * 8, LANES), tall[...])
        products[pl.ds(0, ROWS)] = out.reshape(ROWS, 8, 2 * LANES)
        turned = []
        for k in range(ROWS):
            both = products[k]
            tile = both[:, :LANES] - sign * other_part(both[:, LANES:])
            cosine, sine = down[0, k : k + 1, :], sign * down[1, k : k + 1, :]
            turned.append(tile_turn(tile, cosine, sine))
        values = tile_fft(turned, sign, 1)
        for r in range(ROWS):
            put_b[n, r] = values[r]
        send("row", put_b.at[n], got_b.at[n], SENDB + n)
        got_b[n, row] = put_b[n, row]

    def send_rows(n):
        whole("row", got_b.at[n], SENDB + n).wait_recv()
        put_c[n] = got_b[n].reshape(WIDE, LANES).T.reshape(COLS, 8, WIDE)
        send("col", put_c.at[n], got_c.at[n], SENDC + n)
        got_c[n, col] = put_c[n, col]

    def grow(n):
        whole("col", got_c.at[n], SENDC + n).wait_recv()
        def keep(h, rows):
            part = pl.ds(WIDE * h, WIDE)
            for s in range(COLS // 2):
                grown[n, h, s] = rows[s] * across[n, s : s + 1, part]

        spectrum_of([got_c[n, c] for c in range(COLS)], keep)

    def turn_columns(h):
        whole("col", got2.at[h], SEND2 + h).wait_recv()
        turned = got2[h].reshape(LANES, LANES).T
        for r in range(ROWS):
            put3[h, r] = turned[4 * r : 4 * r + 4]
        send("row", put3.at[h], got3.at[h], SEND3 + h)
        got3[h, row] = put3[h, row]

    def two_blocks(ref, t):
        return jnp.concatenate([ref[2 * t], ref[2 * t + 1]], axis=0)

    def forward_down(h):
        whole("row", got3.at[h], SEND3 + h).wait_recv()
        values = fft_down([two_blocks(got3.at[h], t) for t in range(TILES)], sign)
        for k in range(TILES):
            tiles[k] = tile_turn(values[k], turn2[0, k], -turn2[1, k])
        out = dot_tall(tiles[...].reshape(LANES, LANES), tall[...])
        products[pl.ds(0, TILES)] = out.reshape(TILES, 8, 2 * LANES)
        for k in range(TILES):
            both = products[k]
            spectra[h, k] = both[:, :LANES] + sign * other_part(both[:, LANES:])

    special = sublane() % 4 == jnp.where(row + col == 0, 2, -1)

    def backward_down(n, h):
        parts = 2 if n == 0 and h == 0 else 1
        for k in range(TILES):
            wave = spectra[h, k]
            pair[k] = tables[3 * h + n, k] * wave
            if parts == 2:
                both = jnp.where(sublane() % 2 == 0, wave, roll_rows(wave, 1))
                pair[TILES + k] = tables[2, k] * both
        block = pair[pl.ds(0, parts * TILES)].reshape(parts * LANES, LANES)
        out = dot_tall(block, tall[...])
        products[pl.ds(0, parts * TILES)] = out.reshape(parts * TILES, 8, 2 * LANES)
        for m in reversed(range(parts)):
            turned = []
            for k in range(TILES):
                both = products[m * TILES + k]
                tile = both[:, :LANES] - sign * other_part(both[:, LANES:])
                turned.append(tile_turn(tile, turn2[0, k], turn2[1, k]))
            values = fft_up(turned, sign)
            for t in range(TILES):
                value = values[t]
                if m == 1:
                    extra[t] = value
                    continue
                if h == 0:
                    fixed = extra[t] if n == 0 else roll_rows(extra[t], 7)
                    value = jnp.where(special, fixed, value)
                put4[n, h, 2 * t] = value[:4]
                put4[n, h, 2 * t + 1] = value[4:]
        send("row", put4.at[n, h], got4.at[n, h], SEND4 + 2 * n + h)
        got4[n, h, row] = put4[n, h, row]

    def turn_back(n, h):
        whole("row", got4.at[n, h], SEND4 + 2 * n + h).wait_recv()
        block = jnp.concatenate([two_blocks(got4.at[n, h], t) for t in range(TILES)], axis=0)
        put5[n, h] = block.T.reshape(COLS, 8, LANES)
        send("col", put5.at[n, h], got5.at[n, h], SEND5 + 2 * n + h)
        got5[n, h, col] = put5[n, h, col]

    filter_columns(0)
    for k in range(4):
        back[k] = wide.at[k][...].T
    turn_columns(0)
    turn_columns(1)
    filter_columns(1)
    send_rows(0)
    forward_down(0)
    backward_down(0, 0)
    forward_down(1)
    backward_down(0, 1)
    backward_down(1, 0)
    send_rows(1)
    backward_down(1, 1)
    grow(0)
    for n in range(2):
        for h in range(2):
            turn_back(n, h)
    grow(1)

    feed = feed_forcing()
    for n, out in enumerate((s_out, a_out)):
        for h in range(2):
            whole("col", got5.at[n, h], SEND5 + 2 * n + h).wait_recv()
            rows = [
                jnp.concatenate([got5[n, h, 2 * s], got5[n, h, 2 * s + 1]], axis=1) + grown[n, h, s]
                for s in range(COLS // 2)
            ]
            weights = [back[k, pl.ds(WIDE * h, WIDE), :] for k in range(4)]
            rows = half_product(jnp.concatenate(rows, axis=0), weights)
            if h == 0:
                for s in range(COLS // 2):
                    partial[s] = rows[s]
            else:
                for s in range(COLS // 2):
                    partial[s] = partial[s] + rows[s]
        total = [partial[s] for s in range(COLS // 2)]
        values = backward_columns(total, turn1[0], turn1[1])
        for c in range(COLS):
            put6[n, c] = values[c] + feed if n == 0 else values[c]
        send("col", put6.at[n], out, SEND6 + n)
        out[col] = put6[n, col]

    for n, out in enumerate((s_out, a_out)):
        whole("col", out, SEND6 + n).wait_recv()
    for entry in pending:
        whole(*entry).wait_send()


def store_kernel(s_ref, a_ref, s_out, a_out, sems):
    copies = [
        pltpu.make_async_copy(s_ref, s_out, sems.at[0]),
        pltpu.make_async_copy(a_ref, a_out, sems.at[1]),
    ]
    for copy in copies:
        copy.start()
    for copy in copies:
        copy.wait()


def feed_forcing():
    linear = -FEED_RATE
    return FEED_RATE * math.expm1(HALF_STEP * linear) / linear


def on_device(substrate, activator):
    wide, tall, turn1, turn2, down, across = constants()
    shape = pltpu.VMEM((COLS, 8, WIDE), F32)
    held = lambda x: pltpu.with_memory_space_constraint(x, pltpu.HBM)
    anywhere = pl.BlockSpec(memory_space=pltpu.HBM)
    vmem = lambda *shape: pltpu.VMEM(shape, F32)
    by_col, by_tile = (COLS, 8, WIDE), (TILES, 8, LANES)
    by_row = (ROWS, 8, LANES)
    half_col, half_row = (2, COLS, 8, LANES), (2, ROWS, 4, LANES)
    out = pl.pallas_call(
        kernel,
        name="section",
        out_shape=(shape, shape),
        in_specs=[anywhere] * 8,
        out_specs=(pl.BlockSpec(memory_space=pltpu.VMEM),) * 2,
        scratch_shapes=[
            vmem(3, *by_col),
            pltpu.VMEM(wide.shape, BF16),
            pltpu.VMEM(tall.shape, BF16),
            vmem(*turn1.shape),
            vmem(*turn2.shape),
            vmem(*down.shape),
            vmem(*across.shape),
            vmem(5, *by_tile),
            pltpu.VMEM(wide.shape, BF16),
            vmem(*by_col),
            vmem(*half_col),
            vmem(*half_col),
            vmem(*half_row),
            vmem(*half_row),
            vmem(*by_tile),
            vmem(2, *by_tile),
            vmem(2 * TILES, 8, LANES),
            vmem(2 * TILES, 8, 2 * LANES),
            vmem(*by_tile),
            vmem(2, *half_row),
            vmem(2, *half_row),
            vmem(2, *half_col),
            vmem(2, *half_col),
            vmem(2, *by_col),
            vmem(2, *by_row),
            vmem(2, *by_row),
            vmem(2, *by_row),
            vmem(2, *by_row),
            vmem(2, *by_col),
            vmem(2, *by_col),
            vmem(2, 2, COLS // 2, 8, WIDE),
            vmem(COLS // 2, 8, 2 * WIDE),
            pltpu.SemaphoreType.DMA((8,)),
            pltpu.SemaphoreType.DMA((21,)),
            pltpu.SemaphoreType.DMA((21,)),
        ],
        compiler_params=pltpu.CompilerParams(
            collective_id=0, has_side_effects=True, vmem_limit_bytes=20 << 20
        ),
    )(
        held(substrate.reshape(COLS, 8, WIDE)),
        held(activator.reshape(COLS, 8, WIDE)),
        held(jnp.asarray(wide)),
        held(jnp.asarray(tall)),
        held(jnp.asarray(turn1)),
        held(jnp.asarray(turn2)),
        held(jnp.asarray(down)),
        held(jnp.asarray(across)),
    )
    flat = jax.ShapeDtypeStruct(substrate.shape, F32)
    return pl.pallas_call(
        store_kernel,
        name="store",
        out_shape=(flat, flat),
        in_specs=[pl.BlockSpec(memory_space=pltpu.VMEM)] * 2,
        out_specs=(pl.BlockSpec(memory_space=pltpu.HBM),) * 2,
        scratch_shapes=[pltpu.SemaphoreType.DMA((2,))],
    )(*(pltpu.with_memory_space_constraint(x.reshape(substrate.shape), pltpu.VMEM) for x in out))


def solution(mesh):
    spec = P("row", "col")
    return jax.shard_map(
        on_device, mesh=mesh, in_specs=(spec, spec), out_specs=(spec, spec), check_vma=False
    )
```

```python
import math

import jax
import jax.numpy as jnp
import numpy as np
from jax import lax
from jax.experimental import pallas as pl
from jax.experimental.pallas import tpu as pltpu
from jax.sharding import PartitionSpec as P

FEED_RATE = 0.037
KILL_RATE = 0.06
HALF_STEP = 4.0
SUBSTRATE = (4e-07, FEED_RATE)
ACTIVATOR = (2e-07, FEED_RATE + KILL_RATE)
TOTAL = 4096
COLS = 16
ROWS = 32
WIDE = 256
LANES = 128
TILES = ROWS // 2
F32 = jnp.float32
BF16 = jnp.bfloat16


def c_add(a, b):
    im = a[1] if b[1] is None else (b[1] if a[1] is None else a[1] + b[1])
    return (a[0] + b[0], im)


def c_sub(a, b):
    im = a[1] if b[1] is None else (-b[1] if a[1] is None else a[1] - b[1])
    return (a[0] - b[0], im)


def c_conj(a):
    return (a[0], None if a[1] is None else -a[1])


def c_turn(a, numerator, denominator):
    numerator %= denominator
    if numerator == 0:
        return a
    if 4 * numerator == denominator:
        return (jnp.zeros_like(a[0]) if a[1] is None else -a[1], a[0])
    if 4 * numerator == 3 * denominator:
        return (jnp.zeros_like(a[0]) if a[1] is None else a[1], -a[0])
    cosine = math.cos(2.0 * math.pi * numerator / denominator)
    sine = math.sin(2.0 * math.pi * numerator / denominator)
    if a[1] is None:
        return (a[0] * cosine, a[0] * sine)
    return (a[0] * cosine - a[1] * sine, a[0] * sine + a[1] * cosine)


def real_forward(values):
    size = len(values)
    if size == 2:
        return [(values[0] + values[1], None), (values[0] - values[1], None)]
    even, odd = real_forward(values[::2]), real_forward(values[1::2])
    return join_halves(even, odd, size)


def join_halves(even, odd, size, first=0):
    half = size // 2
    out = [None] * (half + 1)
    for k in range(first, half // 2 + 1):
        turned = c_turn(odd[k], -k, size)
        out[k] = c_add(even[k], turned)
        if half - k != k:
            out[half - k] = c_conj(c_sub(even[k], turned))
    return out


def split_halves(spectrum, size, first=0):
    half = size // 2
    even, odd = [None] * (half // 2 + 1), [None] * (half // 2 + 1)
    for k in range(first, half // 2 + 1):
        if k == 0:
            even[k] = (spectrum[0][0] + spectrum[half][0], None)
            odd[k] = (spectrum[0][0] - spectrum[half][0], None)
        elif 2 * k == half:
            even[k] = (2.0 * spectrum[k][0], None)
            odd[k] = (-2.0 * spectrum[k][1], None)
        else:
            other = c_conj(spectrum[half - k])
            even[k] = c_add(spectrum[k], other)
            odd[k] = c_turn(c_sub(spectrum[k], other), k, size)
    return even, odd


def real_backward(spectrum):
    size = 2 * (len(spectrum) - 1)
    if size == 2:
        a, b = spectrum[0][0], spectrum[1][0]
        return [a + b, a - b]
    even, odd = split_halves(spectrum, size)
    even, odd = real_backward(even), real_backward(odd)
    return [x for pair in zip(even, odd) for x in pair]


def roll_rows(tile, shift):
    return pltpu.roll(tile, shift, 0)


def sublane():
    return lax.broadcasted_iota(jnp.int32, (8, LANES), 0)


def part_sign():
    return jnp.where(sublane() % 4 < 2, 1.0, -1.0).astype(F32)


def other_part(tile):
    return jnp.where(sublane() % 4 < 2, roll_rows(tile, 6), roll_rows(tile, 2))


def tile_turn(tile, cosine, signed_sine):
    return tile * cosine - signed_sine * other_part(tile)


def tile_fft(tiles, sign, direction):
    size = len(tiles)
    if size == 1:
        return tiles
    even, odd = tile_fft(tiles[::2], sign, direction), tile_fft(tiles[1::2], sign, direction)
    low, high = [], []
    for k in range(size // 2):
        turned = odd[k]
        if 4 * k == size:
            turned = (-direction * sign) * other_part(turned)
        elif k:
            angle = direction * 2.0 * math.pi * k / size
            turned = tile_turn(turned, math.cos(angle), sign * math.sin(angle))
        low.append(even[k] + turned)
        high.append(even[k] - turned)
    return low + high


def second_turn(tile, k, sign, direction):
    if k == 0:
        return tile
    angle = direction * 2.0 * math.pi * k / ROWS
    lower = sublane() < 4
    cosine = jnp.where(lower, 1.0, math.cos(angle)).astype(F32)
    sine = jnp.where(lower, 0.0, math.sin(angle)).astype(F32)
    return tile_turn(tile, cosine, sign * sine)


def block_sums(tile):
    return jnp.where(sublane() < 4, tile, -tile) + roll_rows(tile, 4)


def fft_down(tiles, sign):
    turned = [second_turn(x, k, sign, -1) for k, x in enumerate(tile_fft(tiles, sign, -1))]
    return [block_sums(x) for x in turned]


def fft_up(tiles, sign):
    turned = [second_turn(block_sums(x), k, sign, 1) for k, x in enumerate(tiles)]
    return tile_fft(turned, sign, 1)


MATRIX = (((1,), (0,)), ((), ()))


def pieces(values):
    top = values.astype(BF16)
    return top, (values - top.astype(F32)).astype(BF16)


def dot_wide(values, high, low):
    top, rest = pieces(values)
    size = values.shape[0]
    both = lax.dot_general(
        jnp.concatenate([top, rest], axis=0), high, MATRIX, preferred_element_type=F32
    )
    corner = lax.dot_general(top, low, MATRIX, preferred_element_type=F32)
    return both[:size] + (both[size:] + corner)


def dot_tall(values, matrix):
    top, rest = pieces(values)
    stacked = jnp.concatenate([top, rest, top], axis=1)
    parts = [
        lax.dot_general(stacked, part, MATRIX, preferred_element_type=F32)
        for part in (matrix[:, :LANES], matrix[:, LANES:])
    ]
    return jnp.concatenate(parts, axis=1)


def forward_columns(values, turn_cos, turn_sin):
    even, odd = real_forward(values[::2]), real_forward(values[1::2])
    spectrum = join_halves(even, odd, COLS, 1)
    rows = [jnp.concatenate([even[0][0], odd[0][0]], axis=1)]
    for k in range(1, COLS // 2):
        re, im = spectrum[k]
        cosine, sine = turn_cos[k : k + 1, :], turn_sin[k : k + 1, :]
        rows.append(jnp.concatenate([re * cosine + im * sine, im * cosine - re * sine], axis=1))
    return jnp.concatenate(rows, axis=0)


def half_product(stacked, weights):
    out = dot_wide(stacked, weights[0], weights[1])
    first = dot_wide(stacked[:16], weights[2], weights[3])
    return [first[:8]] + [out[8 * slot : 8 * slot + 8] for slot in range(1, COLS // 2)]


def backward_columns(products, turn_cos, turn_sin):
    spectrum = [None] * (COLS // 2)
    for k in range(1, COLS // 2):
        re, im = products[k][:, :WIDE], products[k][:, WIDE:]
        cosine, sine = turn_cos[k : k + 1, :], turn_sin[k : k + 1, :]
        spectrum[k] = (re * cosine - im * sine, im * cosine + re * sine)
    even, odd = split_halves(spectrum + [None], COLS, 1)
    even[0], odd[0] = (products[0][:, :WIDE], None), (products[0][:, WIDE:], None)
    even, odd = real_backward(even), real_backward(odd)
    return [x for pair in zip(even, odd) for x in pair]


def squared_wave(index):
    signed = jnp.where(2 * index < TOTAL, index, index - TOTAL).astype(F32)
    angular = (2.0 * math.pi) * signed
    return angular * angular


def forcing_of(wave_number, diffusion, decay_rate):
    linear = -diffusion * wave_number - decay_rate
    return (jnp.exp(HALF_STEP * linear) - 1.0) / linear


def forcings(step, half, row, col):
    column = sublane() % 2
    slot, side = col // 2, col % 2
    within = LANES * side + 4 * row + 2 * half + column
    q = jnp.where(slot == 0, 8 * within, slot + COLS * within)
    p = step + TILES * (sublane() // 4) + ROWS * lax.broadcasted_iota(jnp.int32, (8, LANES), 1)
    row_wave = squared_wave(p)
    wave_number = row_wave + squared_wave(q)
    norm = 1.0 / (TOTAL * TOTAL)
    scale = jnp.where(q == 0, norm, jnp.where(slot == 0, 2.0 * norm, norm)).astype(F32)
    out = [
        -scale * forcing_of(wave_number, *SUBSTRATE),
        scale * forcing_of(wave_number, *ACTIVATOR),
    ]
    if half == 0:
        last = row_wave + (2.0 * math.pi * (TOTAL // 2)) ** 2
        first = -norm * forcing_of(last, *SUBSTRATE)
        out.append(jnp.where(column == 0, first, norm * forcing_of(last, *ACTIVATOR)))
    return out


def column_growth(index, diffusion):
    angular = 2.0 * np.pi * np.where(2 * index < TOTAL, index, index - TOTAL)
    return np.exp(-HALF_STEP * diffusion * angular * angular)


def constants():
    def split(matrix):
        high = matrix.astype(np.float32).astype(BF16)
        return high, (matrix - high.astype(np.float64)).astype(np.float32).astype(BF16)

    def interleave(re, im):
        both = np.stack([re, im], axis=1).reshape(-1, 2, 2, ROWS, 2, 2)
        return both.transpose(0, 4, 2, 3, 1, 5).reshape(re.shape[0], -1)

    j = np.arange(WIDE)
    angle = 2.0 * np.pi * (np.outer(j, j) % WIDE) / WIDE
    cos, sin = np.cos(angle), np.sin(angle)
    pair = interleave(np.concatenate([cos, sin]), np.concatenate([-sin, cos]))
    long = np.arange(2 * WIDE)
    angle = 2.0 * np.pi * (np.outer(long, j) % (2 * WIDE)) / (2 * WIDE)
    cos, sin = np.cos(angle), -np.sin(angle)
    sin[:, 0] = 1.0 - 2.0 * (long % 2)
    single = interleave(cos, sin)
    wide = np.stack([*split(pair), *split(single)])
    i = np.arange(LANES)
    angle = 2.0 * np.pi * (np.outer(i, i) % LANES) / LANES
    high, low = split(np.concatenate([np.cos(angle), np.sin(angle)], axis=1))
    tall = np.concatenate([high, high, low])

    angle = 2.0 * np.pi * np.outer(np.arange(COLS // 2), j) / TOTAL
    turn1 = np.stack([np.cos(angle), np.sin(angle)]).astype(np.float32)
    block, part, _ = np.unravel_index(np.arange(8), (2, 2, 2))
    wave = np.arange(TILES)[:, None] + TILES * block
    angle = 2.0 * np.pi * wave[:, :, None] * i / TOTAL
    sign = np.where(part == 0, 1.0, -1.0)[:, None]
    turn2 = np.stack([np.cos(angle), sign * np.sin(angle)]).astype(np.float32)
    rows = np.arange(ROWS)[:, None] + ROWS * i
    angle = 2.0 * np.pi * np.arange(ROWS)[:, None] * i / TOTAL
    down = [np.cos(angle), np.sin(angle)]
    slot = np.arange(COLS // 2)[:, None]
    q = np.where(slot == 0, 8 * j, slot + COLS * j)
    last = np.where(q == 0, TOTAL // 2, q)
    paired = np.where(slot == 0, 2.0, 1.0)
    across = []
    for diffusion, decay_rate in (SUBSTRATE, ACTIVATOR):
        down.append(column_growth(rows, diffusion) / TOTAL)
        decay = math.exp(-HALF_STEP * decay_rate) / TOTAL
        parts = [
            np.where(q == 0, 1.0, paired) * column_growth(waves, diffusion) * decay
            for waves in (q, last)
        ]
        across.append(interleave(*parts))
    down, across = np.stack(down).astype(np.float32), np.stack(across).astype(np.float32)
    return wide, tall, turn1, turn2, down, across


SEND1, SEND2, SEND3, SEND4, SEND5, SEND6 = 0, 1, 3, 5, 9, 13
SENDA, SENDB, SENDC = 15, 17, 19


def kernel(
    u_hbm, v_hbm, wide_hbm, tall_hbm, turn1_hbm, turn2_hbm, down_hbm, across_hbm, s_out, a_out,
    fields, wide, tall, turn1, turn2, down, across, tables, back,
    got1, put2, got2, put3, got3, tiles, spectra, pair, products, extra,
    put4, got4, put5, got5, put6,
    put_a, got_a, put_b, got_b, put_c, got_c, grown, partial, local_sem, send_sem, recv_sem,
):
    row, col = lax.axis_index("row"), lax.axis_index("col")
    mesh_id = pl.DeviceIdType.MESH

    loads = [
        pltpu.make_async_copy(src, dst, local_sem.at[n])
        for n, (src, dst) in enumerate(
            [
                (u_hbm, fields.at[0]),
                (v_hbm, fields.at[1]),
                (wide_hbm, wide),
                (tall_hbm, tall),
                (turn1_hbm, turn1),
                (turn2_hbm, turn2),
                (down_hbm, down),
                (across_hbm, across),
            ]
        )
    ]
    for load in loads:
        load.start()

    barrier = pltpu.get_barrier_semaphore()

    def greet(axis, me, size):
        def body(peer, carry):
            pl.semaphore_signal(barrier, inc=1, device_id={axis: peer}, device_id_type=mesh_id)
            return carry

        lax.fori_loop(me + 1, size, body, 0)
        lax.fori_loop(0, me, body, 0)

    pending = []

    def piece(axis, peer, source, target, sem):
        return pltpu.make_async_remote_copy(
            src_ref=source,
            dst_ref=target,
            send_sem=send_sem.at[sem],
            recv_sem=recv_sem.at[sem],
            device_id={axis: peer},
            device_id_type=mesh_id,
        )

    def send(axis, source, target, sem):
        me, size = (col, COLS) if axis == "col" else (row, ROWS)

        def body(peer, carry):
            piece(axis, peer, source.at[peer], target.at[me], sem).start()
            return carry

        lax.fori_loop(me + 1, size, body, 0)
        lax.fori_loop(0, me, body, 0)
        pending.append((axis, source, sem))

    def whole(axis, block, sem):
        me, size = (col, COLS) if axis == "col" else (row, ROWS)
        block = block.at[pl.ds(0, size - 1)]
        return piece(axis, lax.rem(me + 1, size), block, block, sem)

    greet("col", col, COLS)
    greet("row", row, ROWS)
    loads[0].wait()
    loads[1].wait()
    fields[2] = fields[0] * fields[1] * fields[1]
    pl.semaphore_wait(barrier, COLS - 1 + ROWS - 1)

    sign = part_sign()

    send("col", fields.at[2], got1, SEND1)
    got1[col] = fields[2, col]

    for n in range(2):
        put_a[n] = fields[n].reshape(LANES, WIDE).T.reshape(ROWS, 8, LANES)
        send("row", put_a.at[n], got_a.at[n], SENDA + n)
        got_a[n, row] = put_a[n, row]

    def fill(step, carry):
        for half in range(2):
            for n, table in enumerate(forcings(step, half, row, col)):
                tables[3 * half + n, step] = table
        return carry

    lax.fori_loop(0, TILES, fill, 0)
    for load in loads[2:]:
        load.wait()

    def spectrum_of(values, keep):
        stacked = forward_columns(values, turn1[0], turn1[1])
        for h in range(2):
            part = pl.ds(WIDE * h, WIDE)
            keep(h, half_product(stacked, [wide[k, :, part] for k in range(4)]))

    whole("col", got1, SEND1).wait_recv()
    def send_half(h, rows):
        for c in range(COLS):
            start = LANES * (c % 2)
            put2[h, c] = rows[c // 2][:, start : start + LANES]
        send("col", put2.at[h], got2.at[h], SEND2 + h)
        got2[h, col] = put2[h, col]

    spectrum_of([got1[c] for c in range(COLS)], send_half)

    def filter_columns(n):
        whole("row", got_a.at[n], SENDA + n).wait_recv()
        values = tile_fft([got_a[n, r] for r in range(ROWS)], sign, -1)
        for k in range(ROWS):
            cosine, sine = down[0, k : k + 1, :], sign * down[1, k : k + 1, :]
            pair[k] = tile_turn(values[k], cosine, -sine)
        out = dot_tall(pair[...].reshape(ROWS * 8, LANES), tall[...])
        products[pl.ds(0, ROWS)] = out.reshape(ROWS, 8, 2 * LANES)
        for k in range(ROWS):
            both = products[k]
            wave = both[:, :LANES] + sign * other_part(both[:, LANES:])
            pair[k] = wave * down[2 + n, k : k + 1, :]
        out = dot_tall(pair[...].reshape(ROWS * 8, LANES), tall[...])
        products[pl.ds(0, ROWS)] = out.reshape(ROWS, 8, 2 * LANES)
        turned = []
        for k in range(ROWS):
            both = products[k]
            tile = both[:, :LANES] - sign * other_part(both[:, LANES:])
            cosine, sine = down[0, k : k + 1, :], sign * down[1, k : k + 1, :]
            turned.append(tile_turn(tile, cosine, sine))
        values = tile_fft(turned, sign, 1)
        for r in range(ROWS):
            put_b[n, r] = values[r]
        send("row", put_b.at[n], got_b.at[n], SENDB + n)
        got_b[n, row] = put_b[n, row]

    def send_rows(n):
        whole("row", got_b.at[n], SENDB + n).wait_recv()
        put_c[n] = got_b[n].reshape(WIDE, LANES).T.reshape(COLS, 8, WIDE)
        send("col", put_c.at[n], got_c.at[n], SENDC + n)
        got_c[n, col] = put_c[n, col]

    def grow(n):
        whole("col", got_c.at[n], SENDC + n).wait_recv()
        def keep(h, rows):
            part = pl.ds(WIDE * h, WIDE)
            for s in range(COLS // 2):
                grown[n, h, s] = rows[s] * across[n, s : s + 1, part]

        spectrum_of([got_c[n, c] for c in range(COLS)], keep)

    def turn_columns(h):
        whole("col", got2.at[h], SEND2 + h).wait_recv()
        turned = got2[h].reshape(LANES, LANES).T
        for r in range(ROWS):
            put3[h, r] = turned[4 * r : 4 * r + 4]
        send("row", put3.at[h], got3.at[h], SEND3 + h)
        got3[h, row] = put3[h, row]

    def two_blocks(ref, t):
        return jnp.concatenate([ref[2 * t], ref[2 * t + 1]], axis=0)

    def forward_down(h):
        whole("row", got3.at[h], SEND3 + h).wait_recv()
        values = fft_down([two_blocks(got3.at[h], t) for t in range(TILES)], sign)
        for k in range(TILES):
            tiles[k] = tile_turn(values[k], turn2[0, k], -turn2[1, k])
        out = dot_tall(tiles[...].reshape(LANES, LANES), tall[...])
        products[pl.ds(0, TILES)] = out.reshape(TILES, 8, 2 * LANES)
        for k in range(TILES):
            both = products[k]
            spectra[h, k] = both[:, :LANES] + sign * other_part(both[:, LANES:])

    def backward_down(n, h):
        def lifted(scaled):
            for k in range(TILES):
                pair[k] = scaled(k)
            block = pair[pl.ds(0, TILES)].reshape(LANES, LANES)
            products[pl.ds(0, TILES)] = dot_tall(block, tall[...]).reshape(TILES, 8, 2 * LANES)
            turned = []
            for k in range(TILES):
                both = products[k]
                tile = both[:, :LANES] - sign * other_part(both[:, LANES:])
                turned.append(tile_turn(tile, turn2[0, k], turn2[1, k]))
            return fft_up(turned, sign)

        values = lifted(lambda k: tables[3 * h + n, k] * spectra[h, k])
        for t in range(TILES):
            put4[n, h, 2 * t] = values[t][:4]
            put4[n, h, 2 * t + 1] = values[t][4:]

        def last_column(k):
            wave = spectra[h, k]
            return tables[2, k] * jnp.where(sublane() % 2 == 0, wave, roll_rows(wave, 1))

        if h == 0:

            @pl.when(row + col == 0)
            def _():
                if n == 0:
                    for t, value in enumerate(lifted(last_column)):
                        extra[t] = value
                for t in range(TILES):
                    fixed = extra[t] if n == 0 else roll_rows(extra[t], 7)
                    value = jnp.where(sublane() % 4 == 2, fixed, two_blocks(put4.at[n, h], t))
                    put4[n, h, 2 * t] = value[:4]
                    put4[n, h, 2 * t + 1] = value[4:]

        send("row", put4.at[n, h], got4.at[n, h], SEND4 + 2 * n + h)
        got4[n, h, row] = put4[n, h, row]

    def turn_back(n, h):
        whole("row", got4.at[n, h], SEND4 + 2 * n + h).wait_recv()
        block = jnp.concatenate([two_blocks(got4.at[n, h], t) for t in range(TILES)], axis=0)
        put5[n, h] = block.T.reshape(COLS, 8, LANES)
        send("col", put5.at[n, h], got5.at[n, h], SEND5 + 2 * n + h)
        got5[n, h, col] = put5[n, h, col]

    filter_columns(0)
    for k in range(4):
        back[k] = wide.at[k][...].T
    turn_columns(0)
    turn_columns(1)
    filter_columns(1)
    send_rows(0)
    forward_down(0)
    backward_down(0, 0)
    forward_down(1)
    backward_down(0, 1)
    backward_down(1, 0)
    send_rows(1)
    backward_down(1, 1)
    grow(0)
    for n in range(2):
        for h in range(2):
            turn_back(n, h)
    grow(1)

    feed = feed_forcing()
    for n, out in enumerate((s_out, a_out)):
        for h in range(2):
            whole("col", got5.at[n, h], SEND5 + 2 * n + h).wait_recv()
            rows = [
                jnp.concatenate([got5[n, h, 2 * s], got5[n, h, 2 * s + 1]], axis=1) + grown[n, h, s]
                for s in range(COLS // 2)
            ]
            weights = [back[k, pl.ds(WIDE * h, WIDE), :] for k in range(4)]
            rows = half_product(jnp.concatenate(rows, axis=0), weights)
            if h == 0:
                for s in range(COLS // 2):
                    partial[s] = rows[s]
            else:
                for s in range(COLS // 2):
                    partial[s] = partial[s] + rows[s]
        total = [partial[s] for s in range(COLS // 2)]
        values = backward_columns(total, turn1[0], turn1[1])
        for c in range(COLS):
            put6[n, c] = values[c] + feed if n == 0 else values[c]
        send("col", put6.at[n], out, SEND6 + n)
        out[col] = put6[n, col]

    for n, out in enumerate((s_out, a_out)):
        whole("col", out, SEND6 + n).wait_recv()
    for entry in pending:
        whole(*entry).wait_send()


def store_kernel(s_ref, a_ref, s_out, a_out, sems):
    copies = [
        pltpu.make_async_copy(s_ref, s_out, sems.at[0]),
        pltpu.make_async_copy(a_ref, a_out, sems.at[1]),
    ]
    for copy in copies:
        copy.start()
    for copy in copies:
        copy.wait()


def feed_forcing():
    linear = -FEED_RATE
    return FEED_RATE * math.expm1(HALF_STEP * linear) / linear


def on_device(substrate, activator):
    wide, tall, turn1, turn2, down, across = constants()
    shape = pltpu.VMEM((COLS, 8, WIDE), F32)
    held = lambda x: pltpu.with_memory_space_constraint(x, pltpu.HBM)
    anywhere = pl.BlockSpec(memory_space=pltpu.HBM)
    vmem = lambda *shape: pltpu.VMEM(shape, F32)
    by_col, by_tile = (COLS, 8, WIDE), (TILES, 8, LANES)
    by_row = (ROWS, 8, LANES)
    half_col, half_row = (2, COLS, 8, LANES), (2, ROWS, 4, LANES)
    out = pl.pallas_call(
        kernel,
        name="section",
        out_shape=(shape, shape),
        in_specs=[anywhere] * 8,
        out_specs=(pl.BlockSpec(memory_space=pltpu.VMEM),) * 2,
        scratch_shapes=[
            vmem(3, *by_col),
            pltpu.VMEM(wide.shape, BF16),
            pltpu.VMEM(tall.shape, BF16),
            vmem(*turn1.shape),
            vmem(*turn2.shape),
            vmem(*down.shape),
            vmem(*across.shape),
            vmem(5, *by_tile),
            pltpu.VMEM(wide.shape, BF16),
            vmem(*by_col),
            vmem(*half_col),
            vmem(*half_col),
            vmem(*half_row),
            vmem(*half_row),
            vmem(*by_tile),
            vmem(2, *by_tile),
            vmem(2 * TILES, 8, LANES),
            vmem(2 * TILES, 8, 2 * LANES),
            vmem(*by_tile),
            vmem(2, *half_row),
            vmem(2, *half_row),
            vmem(2, *half_col),
            vmem(2, *half_col),
            vmem(2, *by_col),
            vmem(2, *by_row),
            vmem(2, *by_row),
            vmem(2, *by_row),
            vmem(2, *by_row),
            vmem(2, *by_col),
            vmem(2, *by_col),
            vmem(2, 2, COLS // 2, 8, WIDE),
            vmem(COLS // 2, 8, 2 * WIDE),
            pltpu.SemaphoreType.DMA((8,)),
            pltpu.SemaphoreType.DMA((21,)),
            pltpu.SemaphoreType.DMA((21,)),
        ],
        compiler_params=pltpu.CompilerParams(
            collective_id=0, has_side_effects=True, vmem_limit_bytes=20 << 20
        ),
    )(
        held(substrate.reshape(COLS, 8, WIDE)),
        held(activator.reshape(COLS, 8, WIDE)),
        held(jnp.asarray(wide)),
        held(jnp.asarray(tall)),
        held(jnp.asarray(turn1)),
        held(jnp.asarray(turn2)),
        held(jnp.asarray(down)),
        held(jnp.asarray(across)),
    )
    flat = jax.ShapeDtypeStruct(substrate.shape, F32)
    return pl.pallas_call(
        store_kernel,
        name="store",
        out_shape=(flat, flat),
        in_specs=[pl.BlockSpec(memory_space=pltpu.VMEM)] * 2,
        out_specs=(pl.BlockSpec(memory_space=pltpu.HBM),) * 2,
        scratch_shapes=[pltpu.SemaphoreType.DMA((2,))],
    )(*(pltpu.with_memory_space_constraint(x.reshape(substrate.shape), pltpu.VMEM) for x in out))


def solution(mesh):
    spec = P("row", "col")
    return jax.shard_map(
        on_device, mesh=mesh, in_specs=(spec, spec), out_specs=(spec, spec), check_vma=False
    )
```
